256 devices in a mesh: batch: 8 (over y, z_lo), space: 32 (over x, z_hi, core).
Axes of the slice: x: 4, y: 4, z: 8 (z_hi: 4, z_lo: 2; z = z_hi * 2 + z_lo), core: 2. Of those that a mesh axis runs over, the one named last changes fastest.
Arguments:
- features: bfloat16 [8, 160, 64, 512], P('batch', 'space'), may hold values from -6 to 6
- cotangent: bfloat16 [8, 160, 64, 512], P('batch', 'space'), may hold values from -6 to 6
- brick_count: int32 [8, 32], P('batch', 'space'), may hold values from 1 to 5, as said below
- destination: int32 [8, 160], P('batch', 'space'), may hold values from -1 to 63, as said below
- neighbours: int32 [8, 26, 160], P('batch', None, 'space'), may hold values from -1 to 4, as said below
- kernel_one: bfloat16 [64, 1728], replicated, may hold values from -0.15625 to 0.15625
- kernel_two: bfloat16 [64, 1728], replicated, may hold values from -0.15625 to 0.15625
Outputs:
- block_output: bfloat16 [8, 64, 64, 512], P('batch', 'space')
- grad_features: bfloat16 [8, 160, 64, 512], P('batch', 'space')
- grad_kernel_one: float32 [64, 1728], replicated
- grad_kernel_two: float32 [64, 1728], replicated
The draws below stay inside these ranges and needn't reach their ends.
Inputs may be any that keep to these rules, and one draw needn't show every extreme that they name: `brick_count`: A volume holds at most 2 times the devices of space active bricks; some device holds exactly 5. `destination`: -1 exactly on inactive slots. A device's first min(count, 2) bricks go to its own work slots 0, 1, ... in order; its brick in slot 2 + k (k = 0, 1, 2) goes to a work slot of device (s + 1 + k) mod 32; every work slot receives at most one brick, every device receives at most one brick, and a receiving device's own bricks fill its slots below the received one. In every volume some device receives a brick in its work slot 1. `neighbours`: entries of inactive slots are -1; an entry is never the slot of an inactive brick. Bricks sit on a grid of 3 x 3 positions per device, and the offset along the first cell axis is the offset in the device index.
All inputs are finite; a program needn't handle non-finite values.
Results may differ from the reference program's by a relative error of at most 0.0041.
Values may be sent and summed in bfloat16 or wider, within the bound.
A program may use at most 128 MiB of HBM per device.

```python
import math
from functools import partial
import jax
import jax.numpy as jnp
from jax import lax

C = 64
EDGE = 8
WORK_CAP = 2
HOME_CAP = 5
SIDE = 3
CELLS = 512
GROUPS = 8
SLOTS = 160
N_SPACE = 32


def volume_tables(volume_key):
    devices = N_SPACE
    key_list = jax.random.split(volume_key, 4)
    device_ids = jnp.arange(devices, dtype=jnp.int32)
    slot_ids = jnp.arange(HOME_CAP, dtype=jnp.int32)
    rotation = jax.random.randint(key_list[0], (), 0, devices, dtype=jnp.int32)
    order = ((device_ids + rotation) % devices).astype(jnp.int32)
    rank = ((device_ids - rotation) % devices).astype(jnp.int32)
    leaders = jnp.arange(devices // 4, dtype=jnp.int32)
    extra = jax.random.randint(key_list[1], (devices // 4,), 1, 4, dtype=jnp.int32)
    extra = jnp.where(leaders == 0, 3, extra)
    light = jax.random.randint(key_list[2], (devices,), 1, WORK_CAP, dtype=jnp.int32)
    light = jnp.where(rank == 1, WORK_CAP - 1, light)
    member = rank % 4
    team = rank // 4
    counts = jnp.where(member == 0, WORK_CAP + extra[team], light).astype(jnp.int32)
    kept = slot_ids[None, :] < jnp.minimum(counts, WORK_CAP)[:, None]
    surplus = (member == 0)[:, None] & (slot_ids[None, :] >= WORK_CAP) & (slot_ids[None, :] < counts[:, None])
    partner = order[jnp.clip(team[:, None] * 4 + 1 + slot_ids[None, :] - WORK_CAP, 0, devices - 1)]
    moved = partner * WORK_CAP + counts[partner]
    dests = jnp.where(kept, device_ids[:, None] * WORK_CAP + slot_ids[None, :], jnp.where(surplus, moved, -1))

    def one_place(device_number):
        return jax.random.permutation(jax.random.fold_in(key_list[3], device_number), SIDE * SIDE).astype(jnp.int32)
    places = jax.vmap(one_place)(device_ids)
    lookup = jnp.argsort(places, axis=1).astype(jnp.int32)
    spots = places[:, :HOME_CAP]
    entries = []
    for along_first in (-1, 0, 1):
        for along_second in (-1, 0, 1):
            for along_third in (-1, 0, 1):
                if (along_first, along_second, along_third) == (0, 0, 0):
                    continue
                other = device_ids[:, None] + along_first
                row_pos = spots // SIDE + along_second
                col_pos = spots % SIDE + along_third
                inside = (other >= 0) & (other < devices) & (row_pos >= 0) & (row_pos < SIDE) & (col_pos >= 0) & (col_pos < SIDE)
                other_clip = jnp.clip(other, 0, devices - 1)
                spot_clip = jnp.clip(row_pos, 0, SIDE - 1) * SIDE + jnp.clip(col_pos, 0, SIDE - 1)
                found = lookup[other_clip, spot_clip]
                live = inside & (found < counts[other_clip]) & (slot_ids[None, :] < counts[:, None])
                entries.append(jnp.where(live, found, -1))
    table = jnp.stack(entries).reshape(26, devices * HOME_CAP)
    return (counts, dests.reshape(-1).astype(jnp.int32), table.astype(jnp.int32))


def layout_tables(key):
    base = jax.random.fold_in(key, 17)
    volume_keys = jax.vmap(jax.random.fold_in, in_axes=(None, 0))(base, jnp.arange(GROUPS))
    return jax.vmap(volume_tables)(volume_keys)


def draw_brick_count(key, part):
    return layout_tables(key)[0].astype(jnp.int32)


def draw_destination(key, part):
    return layout_tables(key)[1].astype(jnp.int32)


def draw_neighbours(key, part):
    return layout_tables(key)[2].astype(jnp.int32)


def shard_levels(key, extent, cuts, smallest, high):
    loudness, own = 1.0, jax.random.fold_in(key, 6)
    for axis_at, blocks in cuts:
        heights = jnp.exp(jax.random.uniform(jax.random.fold_in(own, axis_at), (blocks,), jnp.float32, smallest / len(cuts), high / len(cuts)))
        loudness = loudness * jnp.repeat(heights, extent[axis_at] // blocks).reshape([-1 if axis == axis_at else 1 for axis in range(len(extent))])
    return loudness


def normal_values(own_key, dims, scale, limit, shards=(), kind=jnp.bfloat16):
    drawn = scale * jax.random.normal(own_key, dims, jnp.float32)
    if shards:
        drawn = drawn * shard_levels(own_key, dims, shards, -0.22, 0.18)
    return jnp.clip(drawn, -limit, limit).astype(kind)


def setup_inputs(seed: int = 0) -> dict:
    keys = jax.random.split(jax.random.key(seed), 8)
    features = normal_values(keys[0], (GROUPS, SLOTS, C, CELLS), 1.0, 6.0, ((0, 8), (1, 32)))
    cotangent = normal_values(keys[1], (GROUPS, SLOTS, C, CELLS), 1.0, 6.0, ((0, 8), (1, 32)))
    brick_count = draw_brick_count(jax.random.fold_in(keys[7], 71), 0)
    destination = draw_destination(jax.random.fold_in(keys[7], 71), 0)
    neighbours = draw_neighbours(jax.random.fold_in(keys[7], 71), 0)
    kernel_one = normal_values(keys[5], (C, 27 * C), (27 * C) ** -0.5, 0.15625)
    kernel_two = normal_values(keys[6], (C, 27 * C), (27 * C) ** -0.5, 0.15625)
    return {"features": features, "cotangent": cotangent, "brick_count": brick_count, "destination": destination, "neighbours": neighbours, "kernel_one": kernel_one, "kernel_two": kernel_two}


def cut_side(region, axis_number, offset, margin_width):
    if offset < 0:
        return lax.slice_in_dim(region, EDGE - margin_width, EDGE, axis=axis_number)
    if offset > 0:
        return lax.slice_in_dim(region, 0, margin_width, axis=axis_number)
    return region

def pick_rows(source, slot_index):
    present = slot_index >= 0
    chosen = jnp.take(source, jnp.maximum(slot_index, 0).astype(jnp.int32), axis=0)
    shaped = present.reshape((-1,) + (1,) * (source.ndim - 1))
    return jnp.where(shaped, chosen, jnp.zeros_like(chosen))

def assemble(home_block, from_lower, from_upper, link_table, margin_width):
    sources = (from_lower, home_block, from_upper)
    slab_list = []
    for along_first in (-1, 0, 1):
        row_list = []
        for along_second in (-1, 0, 1):
            pieces = []
            for along_third in (-1, 0, 1):
                number = 9 * (along_first + 1) + 3 * (along_second + 1) + (along_third + 1)
                if number == 13:
                    region = home_block
                else:
                    position = number if number < 13 else number - 1
                    region = pick_rows(sources[along_first + 1], link_table[position])
                region = cut_side(region, 3, along_second, margin_width)
                region = cut_side(region, 4, along_third, margin_width)
                pieces.append(region)
            row_list.append(jnp.concatenate(pieces, axis=4))
        slab_list.append(jnp.concatenate(row_list, axis=3))
    return jnp.concatenate(slab_list, axis=2)

def plane_columns(flat_cells, side_len, plane_tap, negate, first_cell, stretch):
    pieces = []
    for row_tap in range(3):
        for column in range(3):
            offset = (plane_tap - 1) * side_len * side_len + (row_tap - 1) * side_len + (column - 1)
            if negate:
                offset = -offset
            pieces.append(lax.slice_in_dim(flat_cells, first_cell + offset, first_cell + offset + stretch, axis=1))
    return jnp.concatenate(pieces, axis=0)

def conv_region(flat_cells, kernel, side_len, negate):
    channels = flat_cells.shape[0]
    first_cell = side_len * side_len + side_len + 1
    stretch = side_len ** 3 - 2 * first_cell
    summed = jnp.zeros((kernel.shape[0], stretch), jnp.float32)
    for plane_tap in range(3):
        columns = plane_columns(flat_cells, side_len, plane_tap, negate, first_cell, stretch).astype(jnp.float32)
        part_kernel = kernel[:, plane_tap * 9 * channels:(plane_tap + 1) * 9 * channels].astype(jnp.float32)
        summed = summed + jnp.dot(part_kernel, columns, preferred_element_type=jnp.float32)
    spread = jnp.pad(summed, ((0, 0), (first_cell, first_cell)))
    volume = spread.reshape(-1, side_len, side_len, side_len)[:, 1:-1, 1:-1, 1:-1]
    return volume.reshape(volume.shape[0], -1)

def kernel_grad(flat_cells, inner_grad, side_len):
    channels = flat_cells.shape[0]
    margin_width = (side_len - EDGE) // 2
    first_cell = side_len * side_len + side_len + 1
    stretch = side_len ** 3 - 2 * first_cell
    grid = inner_grad.reshape(channels, EDGE, EDGE, EDGE)
    framed = jnp.pad(grid, ((0, 0), (margin_width, margin_width), (margin_width, margin_width), (margin_width, margin_width)))
    window = lax.slice_in_dim(framed.reshape(channels, -1), first_cell, first_cell + stretch, axis=1).astype(jnp.float32)
    parts = []
    for plane_tap in range(3):
        columns = plane_columns(flat_cells, side_len, plane_tap, False, first_cell, stretch).astype(jnp.float32)
        parts.append(lax.dot_general(window, columns, (((1,), (1,)), ((), ())), preferred_element_type=jnp.float32))
    return jnp.concatenate(parts, axis=1)

def flip_kernel(kernel):
    channels = kernel.shape[0]
    return kernel.reshape(channels, 27, channels).transpose(2, 1, 0).reshape(channels, 27 * channels)

def pad_field(field, link_table, margin_width):
    devices, slots_here, channels = (field.shape[0], field.shape[1], field.shape[2])
    cubes = field.reshape(devices, slots_here, channels, EDGE, EDGE, EDGE)
    empty = jnp.zeros_like(cubes[:1, :, :, :margin_width])
    lower = jnp.concatenate([empty, cubes[:-1, :, :, EDGE - margin_width:]], axis=0)
    upper = jnp.concatenate([cubes[1:, :, :, :margin_width], empty], axis=0)
    tables = link_table.reshape(26, devices, slots_here).transpose(1, 0, 2)
    padded = jax.vmap(partial(assemble, margin_width=margin_width))(cubes, lower, upper, tables)
    return padded.reshape(devices * slots_here, channels, -1)

def by_blocks(function, initial, arrays):
    brick_total = arrays[0].shape[0]
    blocked = tuple((member.reshape((brick_total // 8, 8) + member.shape[1:]) for member in arrays))

    def visit(running, block_items):
        grads, outputs = jax.vmap(function)(*block_items)
        return (running + lax.optimization_barrier(jnp.sum(grads, axis=0)), outputs)
    summed_grad, stacked = lax.scan(visit, initial, blocked)
    return (summed_grad, tuple((piece_out.reshape((brick_total,) + piece_out.shape[2:]) for piece_out in stacked)))

def reference(features, cotangent, brick_count, destination, neighbours, kernel_one, kernel_two):
    channels = features.shape[2]
    flip_one = flip_kernel(kernel_one)
    flip_two = flip_kernel(kernel_two)
    side_len = EDGE + 2
    zero_grad = jnp.zeros((channels, 27 * channels), jnp.float32)

    def one_volume(totals, inputs):
        volume_features, volume_cots, counts, dests, links = inputs
        devices = counts.shape[0]
        slot_ids = jnp.arange(HOME_CAP, dtype=jnp.int32)
        active = (slot_ids[None, :] < counts[:, None]).reshape(-1)
        keep = active[:, None, None]
        masked_x = jnp.where(keep, volume_features, jnp.zeros_like(volume_features))
        masked_dy = jnp.where(keep, volume_cots, jnp.zeros_like(volume_cots))
        shaped = (devices, HOME_CAP, channels, CELLS)
        padded_x = pad_field(masked_x.reshape(shaped), links, 1)

        def first_section(cells_x):
            pre = conv_region(cells_x, kernel_one, side_len, False)
            return (zero_grad, (pre, jax.nn.silu(pre).astype(jnp.bfloat16)))
        unused_grad, (pre_all, hidden_all) = by_blocks(first_section, zero_grad, (padded_x,))
        hidden_all = jnp.where(keep, hidden_all, jnp.zeros_like(hidden_all))
        padded_h = pad_field(hidden_all.reshape(shaped), links, 1)
        padded_dy = pad_field(masked_dy.reshape(shaped), links, 1)

        def second_section(cells_h, cells_dy, inner_x, inner_dy, pre):
            mixed = conv_region(cells_h, kernel_two, side_len, False)
            out_brick = (inner_x.astype(jnp.float32) + mixed).astype(jnp.bfloat16)
            grad_hidden = conv_region(cells_dy, flip_two, side_len, True)
            sigma = jax.nn.sigmoid(pre)
            grad_pre = (grad_hidden * (sigma * (1.0 + pre * (1.0 - sigma)))).astype(jnp.bfloat16)
            return (kernel_grad(cells_h, inner_dy, side_len), (out_brick, grad_pre))
        grad_two, (out_all, grad_pre_all) = by_blocks(second_section, zero_grad, (padded_h, padded_dy, masked_x, masked_dy, pre_all))
        out_all = jnp.where(keep, out_all, jnp.zeros_like(out_all))
        grad_pre_all = jnp.where(keep, grad_pre_all, jnp.zeros_like(grad_pre_all))
        padded_g = pad_field(grad_pre_all.reshape(shaped), links, 1)

        def third_section(cells_g, cells_x, inner_g, inner_dy):
            back_term = conv_region(cells_g, flip_one, side_len, True).astype(jnp.bfloat16)
            summed = (inner_dy.astype(jnp.float32) + back_term.astype(jnp.float32)).astype(jnp.bfloat16)
            return (kernel_grad(cells_x, inner_g, side_len), (summed,))
        grad_one, (grad_in,) = by_blocks(third_section, zero_grad, (padded_g, padded_x, grad_pre_all, masked_dy))
        grad_in = jnp.where(keep, grad_in, jnp.zeros_like(grad_in))
        works = devices * WORK_CAP
        targets = jnp.where(active, dests, works).astype(jnp.int32)
        placed = jnp.zeros((works, channels, CELLS), out_all.dtype).at[targets].set(out_all, mode='drop')
        return ((totals[0] + grad_one, totals[1] + grad_two), (placed, grad_in))
    (grad_one, grad_two), (block_output, grad_features) = lax.scan(one_volume, (zero_grad, zero_grad), (features, cotangent, brick_count, destination, neighbours))
    scale = 1.0 / math.sqrt(GROUPS * SLOTS * CELLS)
    return (block_output, grad_features, grad_one * scale, grad_two * scale)
```

```python
import functools
import math

import jax
import jax.numpy as jnp
import numpy as np
from jax import lax
from jax.experimental import pallas as pl
from jax.experimental.pallas import tpu as pltpu
from jax.sharding import PartitionSpec as P

WORK_CAP = 2
HOME = 5
TILES = 4
SPAN = 6
C = 64
LANES = 128
TAPS = 27
MESH = pl.DeviceIdType.MESH
BF = jnp.bfloat16
F32 = jnp.float32


def shift_matrices():
    def column(q, r, blocks):
        m = np.zeros((len(blocks) * LANES, LANES), np.float32)
        for half in range(2):
            for b in range(8):
                for c in range(8):
                    bb, cc = b + q, c + r
                    kind = (2 if not 0 <= cc < 8 else 0) + (1 if not 0 <= bb < 8 else 0)
                    at = blocks.index(kind) * LANES + half * 64 + (bb % 8) * 8 + cc % 8
                    m[at, half * 64 + b * 8 + c] = 1.0
        return m

    s_q = np.concatenate([column(-1, 0, [1, 0]), column(1, 0, [1, 0])], axis=1)
    s_r = np.concatenate([column(0, -1, [0, 2]), column(0, 1, [0, 2])], axis=1)
    s_c = np.concatenate(
        [column(q, r, [1, 0, 2, 3]) for q, r in ((-1, -1), (-1, 1), (1, -1), (1, 1))], axis=1
    )
    return [jnp.asarray(m, BF) for m in (s_q, s_r, s_c)]


def lane_ids(rows):
    return lax.broadcasted_iota(jnp.int32, (rows, LANES), 1)


def swap_halves(v):
    return pltpu.roll(v, 64, 1)


def to_tiles(parts, lo):
    n0, n1, n2, n3 = parts
    return [
        jnp.where(lo, n0, swap_halves(n2)),
        jnp.where(lo, swap_halves(n0), n2),
        jnp.where(lo, n1, swap_halves(n3)),
        jnp.where(lo, swap_halves(n1), n3),
    ]


def from_tiles(tiles, lo):
    f0, f1, f2, f3 = tiles
    return [
        jnp.where(lo, f0, swap_halves(f1)),
        jnp.where(lo, f2, swap_halves(f3)),
        jnp.where(lo, swap_halves(f0), f1),
        jnp.where(lo, swap_halves(f2), f3),
    ]


def pieces(value):
    return [value[:, k * LANES : (k + 1) * LANES] for k in range(TILES)]


def offset_number(p, q, r):
    number = 9 * (p + 1) + 3 * (q + 1) + (r + 1)
    return number if number < 13 else number - 1


def build_columns(tiles_ref, e0_ref, e3_ref, low_ref, up_ref, links_ref, n, t_ref, d_ref, mats):
    s_q, s_r, s_c = mats
    lane = lane_ids(C)
    lo = lane < 64
    row = (lane % 64) // 8
    col = lane % 8

    def slot(p, q, r):
        if (p, q, r) == (0, 0, 0):
            return n
        found = links_ref[0, offset_number(p, q, r), n]
        return jnp.where(found < 0, HOME, found)

    slots = {
        (p, q, r): slot(p, q, r) for p in (-1, 0, 1) for q in (-1, 0, 1) for r in (-1, 0, 1)
    }

    def source(k, q, r):
        if k == 0:
            return jnp.where(lo, low_ref[slots[-1, q, r]], e3_ref[slots[0, q, r]])
        if k == SPAN - 1:
            return jnp.where(lo, e0_ref[slots[0, q, r]], up_ref[slots[1, q, r]])
        return tiles_ref[slots[0, q, r], k - 1]

    zero = jnp.zeros((C, LANES), BF)
    for k in range(SPAN):
        t1 = source(k, 0, 0)
        t2 = jnp.where(row == 0, source(k, 1, 0), jnp.where(row == 7, source(k, -1, 0), zero))
        t3 = jnp.where(col == 7, source(k, 0, -1), jnp.where(col == 0, source(k, 0, 1), zero))
        up_side = jnp.where(col == 7, source(k, -1, -1), jnp.where(col == 0, source(k, -1, 1), zero))
        down_side = jnp.where(col == 7, source(k, 1, -1), jnp.where(col == 0, source(k, 1, 1), zero))
        t4 = jnp.where(row == 7, up_side, jnp.where(row == 0, down_side, zero))
        rows = slice(k * C, (k + 1) * C)
        t_ref[rows, 0:LANES] = t2
        t_ref[rows, LANES : 2 * LANES] = t1
        t_ref[rows, 2 * LANES : 3 * LANES] = t3
        t_ref[rows, 3 * LANES : 4 * LANES] = t4
        d_ref[n, k, 4 * C : 5 * C, :] = t1

    def put(result, order):
        packed = result.astype(BF)
        for place, qr in enumerate(order):
            for k in range(SPAN):
                d_ref[n, k, qr * C : (qr + 1) * C, :] = packed[
                    k * C : (k + 1) * C, place * LANES : (place + 1) * LANES
                ]

    put(jnp.dot(t_ref[:, 0 : 2 * LANES], s_q[...], preferred_element_type=F32), (1, 7))
    put(jnp.dot(t_ref[:, LANES : 3 * LANES], s_r[...], preferred_element_type=F32), (3, 5))
    put(jnp.dot(t_ref[...], s_c[...], preferred_element_type=F32), (0, 2, 6, 8))


def halo_pack(tiles_a, tiles_b, lo):
    down = jnp.where(lo, swap_halves(tiles_a[3]), tiles_b[3])
    back = jnp.where(lo, tiles_b[0], swap_halves(tiles_a[0]))
    return down, back


def neighbours_ring(space):
    me = lax.axis_index("space")
    batch = lax.axis_index("batch")
    return (batch, lax.rem(me + 1, space)), (batch, lax.rem(me + space - 1, space))


def exchange(down_ref, back_ref, low_ref, up_ref, send_sem, recv_sem, space):
    following, previous = neighbours_ring(space)
    forward = pltpu.make_async_remote_copy(
        src_ref=down_ref, dst_ref=low_ref, send_sem=send_sem.at[0], recv_sem=recv_sem.at[0],
        device_id=following, device_id_type=MESH,
    )
    backward = pltpu.make_async_remote_copy(
        src_ref=back_ref, dst_ref=up_ref, send_sem=send_sem.at[1], recv_sem=recv_sem.at[1],
        device_id=previous, device_id_type=MESH,
    )
    return forward, backward


def greet(devices):
    barrier = pltpu.get_barrier_semaphore()
    for device in devices:
        pl.semaphore_signal(barrier, inc=1, device_id=device, device_id_type=MESH)
    return barrier


def first_halo_kernel(space, x_ref, dy_ref, low_ref, up_ref, down_buf, back_buf, send_sem, recv_sem):
    barrier = greet(neighbours_ring(space))
    lo = lane_ids(C) < 64
    for n in range(HOME):
        tx = to_tiles(pieces(x_ref[n]), lo)
        ty = to_tiles(pieces(dy_ref[n]), lo)
        down, back = halo_pack(tx, ty, lo)
        down_buf[n] = down
        back_buf[n] = back
    pl.semaphore_wait(barrier, 2)
    copies = exchange(down_buf, back_buf, low_ref, up_ref, send_sem, recv_sem, space)
    for copy in copies:
        copy.start()
    for copy in copies:
        copy.wait()


def second_halo_kernel(space, down_ref, back_ref, low_ref, up_ref, send_sem, recv_sem):
    barrier = greet(neighbours_ring(space))
    pl.semaphore_wait(barrier, 2)
    copies = exchange(down_ref, back_ref, low_ref, up_ref, send_sem, recv_sem, space)
    for copy in copies:
        copy.start()
    for copy in copies:
        copy.wait()


def unpack_halo(low_in, up_in, lows, ups):
    for n in range(HOME):
        lows[0][n] = low_in[n]
        lows[1][n] = swap_halves(low_in[n])
        ups[0][n] = up_in[n]
        ups[1][n] = swap_halves(up_in[n])
    zero = jnp.zeros((C, LANES), BF)
    for ref in (*lows, *ups):
        ref[HOME] = zero


def clear_last(tiles_ref, e0_ref, e3_ref):
    zero = jnp.zeros((C, LANES), BF)
    for j in range(TILES):
        tiles_ref[HOME, j] = zero
    e0_ref[HOME] = zero
    e3_ref[HOME] = zero


def first_kernel(
    x_ref, dy_ref, low_in, up_in, links_ref, count_ref, k1_ref, f2_ref, sq_ref, sr_ref, sc_ref,
    h_out, g_out, down_out, back_out, sums_out,
    xt, yt, ex0, ex3, ey0, ey3, lx, ly, ux, uy, t_buf, dx, dd, gpad, hpad, acc1, acc2,
):
    lane = lane_ids(C)
    lo = lane < 64
    mats = (sq_ref, sr_ref, sc_ref)
    unpack_halo(low_in, up_in, (lx, ly), (ux, uy))
    clear_last(xt, ex0, ex3)
    clear_last(yt, ey0, ey3)
    zero = jnp.zeros((C, LANES), BF)
    count = count_ref[0, 0]
    for n in range(HOME):
        live = jnp.where(n < count, 1.0, 0.0).astype(F32)
        for src, tiles_ref, e0, e3 in ((x_ref, xt, ex0, ex3), (dy_ref, yt, ey0, ey3)):
            masked = (src[n].astype(F32) * live).astype(BF)
            tiles = to_tiles(pieces(masked), lo)
            for j in range(TILES):
                tiles_ref[n, j] = tiles[j]
            e0[n] = swap_halves(tiles[0])
            e3[n] = swap_halves(tiles[3])
    for ref in (gpad, hpad):
        for j in (0, 1, 6, 7):
            ref[j] = zero
    acc1[...] = jnp.zeros_like(acc1)
    acc2[...] = jnp.zeros_like(acc2)

    def brick(n, _):
        build_columns(xt, ex0, ex3, lx, ux, links_ref, n, t_buf, dx, mats)
        build_columns(yt, ey0, ey3, ly, uy, links_ref, n, t_buf, dd, mats)
        hidden = []
        grads = []
        for j in range(TILES):
            pre = jnp.dot(
                k1_ref[...], dx[n, j : j + 3].reshape(TAPS * C, LANES), preferred_element_type=F32
            )
            grad_hidden = jnp.dot(
                f2_ref[...], dd[n, j : j + 3].reshape(TAPS * C, LANES), preferred_element_type=F32
            )
            sigma = 1.0 / (1.0 + jnp.exp(-pre))
            hid = (pre * sigma).astype(BF)
            gpre = (grad_hidden * (sigma * (1.0 + pre * (1.0 - sigma)))).astype(BF)
            h_out[n, j] = hid
            g_out[n, j] = gpre
            hpad[j + 2] = hid
            gpad[j + 2] = gpre
            hidden.append(hid)
            grads.append(gpre)
        down, back = halo_pack(hidden, grads, lo)
        down_out[n] = down
        back_out[n] = back
        for acc, cols, pad, flip in ((acc1, dx, gpad, False), (acc2, dd, hpad, True)):
            total = acc[...]
            for k in (0, 2, 4):
                left = jnp.concatenate([cols[n, k], cols[n, k + 1]], axis=1)

                def right(at):
                    if flip:
                        return jnp.concatenate([pad[at + 1], pad[at], zero, pad[at + 2]], axis=0)
                    return jnp.concatenate([pad[at], pad[at + 1], pad[at + 2], zero], axis=0)

                both = jnp.concatenate([right(k), right(k + 1)], axis=1)
                total = total + lax.dot_general(
                    left, both, (((1,), (1,)), ((), ())), preferred_element_type=F32
                )
            acc[...] = total
        return 0

    lax.fori_loop(0, HOME, brick, 0)
    wide = lane_ids(9 * C) < 64
    first_a, first_b = acc1[:, 0:LANES], acc1[:, LANES : 2 * LANES]
    second_a, second_b = acc2[:, 0:LANES], acc2[:, LANES : 2 * LANES]
    sums_out[0 : 9 * C, :] = jnp.where(wide, first_b, second_b).astype(BF)
    sums_out[9 * C : 18 * C, :] = jnp.where(wide, second_a, first_a).astype(BF)
    sums_out[18 * C : 27 * C, :] = jnp.where(wide, first_a, second_a).astype(BF)
    sums_out[27 * C : 2048, :] = jnp.zeros((2048 - 27 * C, LANES), BF)


def second_kernel(
    x_ref, dy_ref, h_ref, g_ref, low_in, up_in, links_ref, count_ref, k2_ref, f1_ref,
    sq_ref, sr_ref, sc_ref, out_ref, grad_ref,
    ht, gt, eh0, eh3, eg0, eg3, lh, lg, uh, ug, t_buf, dh, dg,
):
    lane = lane_ids(C)
    lo = lane < 64
    mats = (sq_ref, sr_ref, sc_ref)
    unpack_halo(low_in, up_in, (lh, lg), (uh, ug))
    clear_last(ht, eh0, eh3)
    clear_last(gt, eg0, eg3)
    count = count_ref[0, 0]
    for n in range(HOME):
        for src, tiles_ref, e0, e3 in ((h_ref, ht, eh0, eh3), (g_ref, gt, eg0, eg3)):
            for j in range(TILES):
                tiles_ref[n, j] = src[n, j]
            e0[n] = swap_halves(src[n, 0])
            e3[n] = swap_halves(src[n, 3])

    def brick(n, _):
        build_columns(ht, eh0, eh3, lh, uh, links_ref, n, t_buf, dh, mats)
        build_columns(gt, eg0, eg3, lg, ug, links_ref, n, t_buf, dg, mats)
        mixed = []
        backs = []
        for j in range(TILES):
            mixed.append(jnp.dot(
                k2_ref[...], dh[n, j : j + 3].reshape(TAPS * C, LANES), preferred_element_type=F32
            ))
            backs.append(jnp.dot(
                f1_ref[...], dg[n, j : j + 3].reshape(TAPS * C, LANES), preferred_element_type=F32
            ))
        live = jnp.where(n < count, 1.0, 0.0).astype(F32)
        for k, (m, b) in enumerate(zip(from_tiles(mixed, lo), from_tiles(backs, lo))):
            lanes = slice(k * LANES, (k + 1) * LANES)
            out_ref[n, :, lanes] = ((x_ref[n, :, lanes].astype(F32) + m) * live).astype(BF)
            term = b.astype(BF).astype(F32)
            grad_ref[n, :, lanes] = ((dy_ref[n, :, lanes].astype(F32) + term) * live).astype(BF)
        return 0

    lax.fori_loop(0, HOME, brick, 0)


def finish_kernel(
    space, scale, s_ref, ob_ref, work_ref, one_ref, two_ref,
    r1, p2, r2, q_buf, a2, chunk, a1, arrived, total,
    s1s, s1r, s2s, s2r, g2s, g2r, g1s, g1r, obs, obr,
):
    batch = lax.axis_index("batch")
    at = lax.axis_index("space")
    y, z_lo = batch // 2, lax.rem(batch, 2)
    x, inner = at // 8, lax.rem(at, 8)
    g = x * 4 + y
    h = z_lo * 8 + inner

    def plane_peer(number):
        return (lax.rem(number, 4) * 2 + z_lo, (number // 4) * 8 + inner)

    def column_peer(number):
        return (y * 2 + number // 8, x * 8 + lax.rem(number, 8))

    def ring(step):
        return (batch, lax.rem(at + space + step, space))

    plane = [plane_peer(lax.rem(g + d, 16)) for d in range(1, 16)]
    column = [column_peer(lax.rem(h + d, 16)) for d in range(1, 16)]
    barrier = greet(plane + column + [ring(-1), ring(-2), ring(-3)])
    pl.semaphore_wait(barrier, 33)

    def start(src, dst, sends, recvs, number, device):
        copy = pltpu.make_async_remote_copy(
            src_ref=src, dst_ref=dst, send_sem=sends.at[number], recv_sem=recvs.at[number],
            device_id=device, device_id_type=MESH,
        )
        copy.start()
        return copy

    scatter = [
        start(s_ref.at[lax.rem(g + d, 16)], r1.at[d - 1], s1s, s1r, d - 1, plane[d - 1])
        for d in range(1, 16)
    ]
    bricks = [
        start(ob_ref.at[WORK_CAP + k], arrived.at[k], obs, obr, k, ring(k + 1)) for k in range(3)
    ]
    acc = s_ref[g].astype(F32)
    for d in range(15):
        scatter[d].wait_recv()
        acc = acc + r1[d].astype(F32)
    p2[...] = acc.reshape(16, 8, LANES)
    column_scatter = [
        start(p2.at[lax.rem(h + d, 16)], r2.at[d - 1], s2s, s2r, d - 1, column[d - 1])
        for d in range(1, 16)
    ]
    piece = p2[h]
    for d in range(15):
        column_scatter[d].wait_recv()
        piece = piece + r2[d]
    q_buf[...] = piece
    a2[h] = piece
    column_gather = [
        start(q_buf, a2.at[h], g2s, g2r, d - 1, column[d - 1]) for d in range(1, 16)
    ]
    for d in range(15):
        column_gather[d].wait_recv()
    whole = a2[...].reshape(LANES, LANES).astype(BF)
    chunk[...] = whole
    a1[g] = whole
    gather = [start(chunk, a1.at[g], g1s, g1r, d - 1, plane[d - 1]) for d in range(1, 16)]
    for k in range(3):
        bricks[k].wait_recv()
    work_ref[0] = ob_ref[0]
    extra = arrived[0].astype(F32) + arrived[1].astype(F32) + arrived[2].astype(F32)
    work_ref[1] = (ob_ref[1].astype(F32) + extra).astype(BF)
    for d in range(15):
        gather[d].wait_recv()
    total[...] = a1[...].reshape(2048, LANES).astype(F32) * scale
    lo = lane_ids(C) < 64

    def block(tap):
        return total[tap * C : (tap + 1) * C, :]

    def swapped(tap):
        return 9 <= tap < 18

    def first_block(tap, low):
        value = block(tap)
        return value if swapped(tap) != low else swap_halves(value)

    def second_block(tap, low):
        value = block(TAPS - 1 - tap)
        return value if swapped(tap) == low else swap_halves(value)

    for tile in range(14):
        tap = 2 * tile
        here = first_block(tap, True)
        there = second_block(tap, True)
        if tap + 1 < TAPS:
            pair = jnp.concatenate([here, first_block(tap + 1, True)], axis=0)
            one_ref[:, tile * LANES : (tile + 1) * LANES] = pair.T[0:C, :]
            two_ref[:, tile * LANES : (tile + 1) * LANES] = jnp.where(
                lo, there, second_block(tap + 1, False)
            )
        else:
            pair = jnp.concatenate([here, here], axis=0)
            one_ref[:, tile * LANES : tile * LANES + C] = pair.T[0:C, 0:C]
            two_ref[:, tile * LANES : tile * LANES + C] = there[:, 0:C]
    for copy in (*scatter, *column_scatter, *column_gather, *gather, *bricks):
        copy.wait_send()


def vmem():
    return pl.BlockSpec(memory_space=pltpu.VMEM)


def smem():
    return pl.BlockSpec(memory_space=pltpu.SMEM)


def bf_scratch(*shape):
    return pltpu.VMEM(shape, BF)


def flip_kernel(kernel):
    channels = kernel.shape[0]
    taps = kernel.reshape(channels, TAPS, channels)[:, ::-1, :]
    return taps.transpose(2, 1, 0).reshape(channels, TAPS * channels)


def field_scratch():
    tiles = [bf_scratch(HOME + 1, TILES, C, LANES)] * 2
    rows = [bf_scratch(HOME + 1, C, LANES)] * 8
    columns = [bf_scratch(SPAN * C, 4 * LANES)] + [bf_scratch(HOME, SPAN, 9 * C, LANES)] * 2
    return tiles + rows + columns


def halo_call(kernel, number, extra, args):
    return pl.pallas_call(
        kernel,
        out_shape=[jax.ShapeDtypeStruct((HOME, C, LANES), BF)] * 2,
        in_specs=[vmem()] * 2,
        out_specs=[vmem()] * 2,
        scratch_shapes=[*extra, pltpu.SemaphoreType.DMA((2,)), pltpu.SemaphoreType.DMA((2,))],
        compiler_params=pltpu.CompilerParams(collective_id=number, has_side_effects=True),
    )(*args)


def shards(space, groups, features, cotangent, brick_count, destination, neighbours, kernel_one, kernel_two):
    x = features[0]
    dy = cotangent[0]
    mats = shift_matrices()
    halo = bf_scratch(HOME, C, LANES)
    low, up = halo_call(functools.partial(first_halo_kernel, space), 0, [halo, halo], (x, dy))
    tile_shape = jax.ShapeDtypeStruct((HOME, TILES, C, LANES), BF)
    halo_shape = jax.ShapeDtypeStruct((HOME, C, LANES), BF)
    local = pltpu.CompilerParams(vmem_limit_bytes=60 * 1024 * 1024)
    hidden, gpre, down, back, sums = pl.pallas_call(
        first_kernel,
        out_shape=[
            tile_shape, tile_shape, halo_shape, halo_shape,
            jax.ShapeDtypeStruct((2048, LANES), BF),
        ],
        in_specs=[vmem()] * 4 + [smem()] * 2 + [vmem()] * 5,
        out_specs=[vmem()] * 5,
        scratch_shapes=field_scratch()
        + [bf_scratch(8, C, LANES)] * 2
        + [pltpu.VMEM((9 * C, 2 * LANES), F32)] * 2,
        compiler_params=local,
    )(x, dy, low, up, neighbours, brick_count, kernel_one, flip_kernel(kernel_two), *mats)
    low, up = halo_call(functools.partial(second_halo_kernel, space), 1, [], (down, back))
    bricks_shape = jax.ShapeDtypeStruct((HOME, C, TILES * LANES), BF)
    out, grad_in = pl.pallas_call(
        second_kernel,
        out_shape=[bricks_shape, bricks_shape],
        in_specs=[vmem()] * 6 + [smem()] * 2 + [vmem()] * 5,
        out_specs=[vmem()] * 2,
        scratch_shapes=field_scratch(),
        compiler_params=local,
    )(x, dy, hidden, gpre, low, up, neighbours, brick_count, kernel_two, flip_kernel(kernel_one), *mats)
    scale = 1.0 / math.sqrt(groups * space * HOME * TILES * LANES)
    grad_shape = jax.ShapeDtypeStruct((C, TAPS * C), F32)
    dma = pltpu.SemaphoreType.DMA
    work, grad_one, grad_two = pl.pallas_call(
        functools.partial(finish_kernel, space, scale),
        out_shape=[
            jax.ShapeDtypeStruct((WORK_CAP, C, TILES * LANES), BF), grad_shape, grad_shape,
        ],
        in_specs=[vmem()] * 2,
        out_specs=[vmem()] * 3,
        scratch_shapes=[
            bf_scratch(15, LANES, LANES),
            pltpu.VMEM((16, 8, LANES), F32),
            pltpu.VMEM((15, 8, LANES), F32),
            pltpu.VMEM((8, LANES), F32),
            pltpu.VMEM((16, 8, LANES), F32),
            bf_scratch(LANES, LANES),
            bf_scratch(16, LANES, LANES),
            bf_scratch(3, C, TILES * LANES),
            pltpu.VMEM((2048, LANES), F32),
        ]
        + [dma((15,))] * 8
        + [dma((3,))] * 2,
        compiler_params=pltpu.CompilerParams(collective_id=2, has_side_effects=True),
    )(sums.reshape(16, LANES, LANES), out)
    return work[None], grad_in[None], grad_one, grad_two


def solution(mesh):
    return jax.shard_map(
        functools.partial(shards, mesh.shape["space"], mesh.shape["batch"]),
        mesh=mesh,
        in_specs=(
            P("batch", "space", None, None),
            P("batch", "space", None, None),
            P("batch", "space"),
            P("batch", "space"),
            P("batch", None, "space"),
            P(),
            P(),
        ),
        out_specs=(P("batch", "space", None, None), P("batch", "space", None, None), P(), P()),
        check_vma=False,
    )
```

```python
import functools
import math

import jax
import jax.numpy as jnp
import numpy as np
from jax import lax
from jax.experimental import pallas as pl
from jax.experimental.pallas import tpu as pltpu
from jax.sharding import PartitionSpec as P

WORK_CAP = 2
HOME = 5
TILES = 4
SPAN = 6
C = 64
LANES = 128
TAPS = 27
VMEM_BYTES = 60 * 1024 * 1024
MESH = pl.DeviceIdType.MESH
BF = jnp.bfloat16
F32 = jnp.float32


def shift_matrices():
    def column(q, r, blocks):
        m = np.zeros((len(blocks) * LANES, LANES), np.float32)
        for half in range(2):
            for b in range(8):
                for c in range(8):
                    bb, cc = b + q, c + r
                    kind = (2 if not 0 <= cc < 8 else 0) + (1 if not 0 <= bb < 8 else 0)
                    at = blocks.index(kind) * LANES + half * 64 + (bb % 8) * 8 + cc % 8
                    m[at, half * 64 + b * 8 + c] = 1.0
        return m

    s_q = np.concatenate([column(-1, 0, [1, 0]), column(1, 0, [1, 0])], axis=1)
    s_r = np.concatenate([column(0, -1, [0, 2]), column(0, 1, [0, 2])], axis=1)
    s_c = np.concatenate(
        [column(q, r, [1, 0, 2, 3]) for q, r in ((-1, -1), (-1, 1), (1, -1), (1, 1))], axis=1
    )
    return [jnp.asarray(m, BF) for m in (s_q, s_r, s_c)]


def lane_ids(rows):
    return lax.broadcasted_iota(jnp.int32, (rows, LANES), 1)


def swap_halves(v):
    return pltpu.roll(v, 64, 1)


def to_tiles(parts, lo):
    n0, n1, n2, n3 = parts
    return [
        jnp.where(lo, n0, swap_halves(n2)),
        jnp.where(lo, swap_halves(n0), n2),
        jnp.where(lo, n1, swap_halves(n3)),
        jnp.where(lo, swap_halves(n1), n3),
    ]


def from_tiles(tiles, lo):
    f0, f1, f2, f3 = tiles
    return [
        jnp.where(lo, f0, swap_halves(f1)),
        jnp.where(lo, f2, swap_halves(f3)),
        jnp.where(lo, swap_halves(f0), f1),
        jnp.where(lo, swap_halves(f2), f3),
    ]


def pieces(value):
    return [value[:, k * LANES : (k + 1) * LANES] for k in range(TILES)]


def offset_number(p, q, r):
    number = 9 * (p + 1) + 3 * (q + 1) + (r + 1)
    return number if number < 13 else number - 1


def build_columns(tiles_ref, e0_ref, e3_ref, low_ref, up_ref, links_ref, n, t_ref, d_ref, mats):
    s_q, s_r, s_c = mats
    lane = lane_ids(C)
    lo = lane < 64
    row = (lane % 64) // 8
    col = lane % 8

    def slot(p, q, r):
        if (p, q, r) == (0, 0, 0):
            return n
        found = links_ref[0, offset_number(p, q, r), n]
        return jnp.where(found < 0, HOME, found)

    slots = {
        (p, q, r): slot(p, q, r) for p in (-1, 0, 1) for q in (-1, 0, 1) for r in (-1, 0, 1)
    }

    def source(k, q, r):
        if k == 0:
            return jnp.where(lo, low_ref[slots[-1, q, r]], e3_ref[slots[0, q, r]])
        if k == SPAN - 1:
            return jnp.where(lo, e0_ref[slots[0, q, r]], up_ref[slots[1, q, r]])
        return tiles_ref[slots[0, q, r], k - 1]

    zero = jnp.zeros((C, LANES), BF)
    for k in range(SPAN):
        t1 = source(k, 0, 0)
        t2 = jnp.where(row == 0, source(k, 1, 0), jnp.where(row == 7, source(k, -1, 0), zero))
        t3 = jnp.where(col == 7, source(k, 0, -1), jnp.where(col == 0, source(k, 0, 1), zero))
        up_side = jnp.where(col == 7, source(k, -1, -1), jnp.where(col == 0, source(k, -1, 1), zero))
        down_side = jnp.where(col == 7, source(k, 1, -1), jnp.where(col == 0, source(k, 1, 1), zero))
        t4 = jnp.where(row == 7, up_side, jnp.where(row == 0, down_side, zero))
        rows = slice(k * C, (k + 1) * C)
        t_ref[rows, 0:LANES] = t2
        t_ref[rows, LANES : 2 * LANES] = t1
        t_ref[rows, 2 * LANES : 3 * LANES] = t3
        t_ref[rows, 3 * LANES : 4 * LANES] = t4
        d_ref[n, k, 4 * C : 5 * C, :] = t1

    def put(result, order):
        packed = result.astype(BF)
        for place, qr in enumerate(order):
            for k in range(SPAN):
                d_ref[n, k, qr * C : (qr + 1) * C, :] = packed[
                    k * C : (k + 1) * C, place * LANES : (place + 1) * LANES
                ]

    put(jnp.dot(t_ref[:, 0 : 2 * LANES], s_q[...], preferred_element_type=F32), (1, 7))
    put(jnp.dot(t_ref[:, LANES : 3 * LANES], s_r[...], preferred_element_type=F32), (3, 5))
    put(jnp.dot(t_ref[...], s_c[...], preferred_element_type=F32), (0, 2, 6, 8))


def halo_pack(tiles_a, tiles_b, lo):
    down = jnp.where(lo, swap_halves(tiles_a[3]), tiles_b[3])
    back = jnp.where(lo, tiles_b[0], swap_halves(tiles_a[0]))
    return down, back


def neighbours_ring(space):
    me = lax.axis_index("space")
    batch = lax.axis_index("batch")
    return (batch, lax.rem(me + 1, space)), (batch, lax.rem(me + space - 1, space))


def exchange(down_ref, back_ref, low_ref, up_ref, send_sem, recv_sem, space):
    following, previous = neighbours_ring(space)
    forward = pltpu.make_async_remote_copy(
        src_ref=down_ref, dst_ref=low_ref, send_sem=send_sem.at[0], recv_sem=recv_sem.at[0],
        device_id=following, device_id_type=MESH,
    )
    backward = pltpu.make_async_remote_copy(
        src_ref=back_ref, dst_ref=up_ref, send_sem=send_sem.at[1], recv_sem=recv_sem.at[1],
        device_id=previous, device_id_type=MESH,
    )
    return forward, backward


def greet(devices):
    barrier = pltpu.get_barrier_semaphore()
    for device in devices:
        pl.semaphore_signal(barrier, inc=1, device_id=device, device_id_type=MESH)
    return barrier


def flip_kernels(k1_ref, k2_ref, f1_ref, f2_ref):
    lo = lane_ids(C) < 64

    def turned(tile):
        lanes = slice(tile * LANES, min((tile + 1) * LANES, TAPS * C))
        stacked = jnp.concatenate([k1_ref[:, lanes], k2_ref[:, lanes]], axis=0).astype(F32)
        if stacked.shape[1] < LANES:
            stacked = jnp.concatenate([stacked, stacked], axis=1)
        return stacked.T

    later = turned(13)
    for tile in range(14):
        here = later[0:C]
        if tile < 13:
            later = turned(12 - tile)
            next_one = later[C : 2 * C]
            lanes = slice(tile * LANES, (tile + 1) * LANES)
            f1_ref[:, lanes] = jnp.where(lo, here, swap_halves(next_one)).astype(BF)
            f2_ref[:, lanes] = jnp.where(lo, swap_halves(here), next_one).astype(BF)
        else:
            lanes = slice(tile * LANES, TAPS * C)
            f1_ref[:, lanes] = here[:, 0:C].astype(BF)
            f2_ref[:, lanes] = swap_halves(here)[:, 0:C].astype(BF)


def first_halo_kernel(
    space, x_ref, dy_ref, k1_ref, k2_ref, low_ref, up_ref, f1_ref, f2_ref,
    down_buf, back_buf, send_sem, recv_sem,
):
    barrier = greet(neighbours_ring(space))
    lo = lane_ids(C) < 64
    for n in range(HOME):
        first_x, first_dy = x_ref[n, :, 0:LANES], dy_ref[n, :, 0:LANES]
        last_x, last_dy = x_ref[n, :, 3 * LANES :], dy_ref[n, :, 3 * LANES :]
        down_buf[n] = jnp.where(lo, swap_halves(last_x), last_dy)
        back_buf[n] = jnp.where(lo, first_dy, swap_halves(first_x))
    pl.semaphore_wait(barrier, 2)
    copies = exchange(down_buf, back_buf, low_ref, up_ref, send_sem, recv_sem, space)
    for copy in copies:
        copy.start()
    flip_kernels(k1_ref, k2_ref, f1_ref, f2_ref)
    for copy in copies:
        copy.wait()


def unpack_halo(low_in, up_in, lows, ups):
    for n in range(HOME):
        lows[0][n] = low_in[n]
        lows[1][n] = swap_halves(low_in[n])
        ups[0][n] = up_in[n]
        ups[1][n] = swap_halves(up_in[n])
    zero = jnp.zeros((C, LANES), BF)
    for ref in (*lows, *ups):
        ref[HOME] = zero


def clear_last(tiles_ref, e0_ref, e3_ref):
    zero = jnp.zeros((C, LANES), BF)
    for j in range(TILES):
        tiles_ref[HOME, j] = zero
    e0_ref[HOME] = zero
    e3_ref[HOME] = zero


def first_kernel(
    x_ref, dy_ref, low_in, up_in, links_ref, count_ref, k1_ref, f2_ref, sq_ref, sr_ref, sc_ref,
    h_out, g_out, down_out, back_out, sums_out,
    xt, yt, ex0, ex3, ey0, ey3, lx, ly, ux, uy, t_buf, dx, dd, gpad, hpad, acc1, acc2,
):
    lane = lane_ids(C)
    lo = lane < 64
    mats = (sq_ref, sr_ref, sc_ref)
    unpack_halo(low_in, up_in, (lx, ly), (ux, uy))
    clear_last(xt, ex0, ex3)
    clear_last(yt, ey0, ey3)
    zero = jnp.zeros((C, LANES), BF)
    count = count_ref[0, 0]
    for n in range(HOME):
        live = jnp.where(n < count, 1.0, 0.0).astype(F32)
        for src, tiles_ref, e0, e3 in ((x_ref, xt, ex0, ex3), (dy_ref, yt, ey0, ey3)):
            masked = (src[n].astype(F32) * live).astype(BF)
            tiles = to_tiles(pieces(masked), lo)
            for j in range(TILES):
                tiles_ref[n, j] = tiles[j]
            e0[n] = swap_halves(tiles[0])
            e3[n] = swap_halves(tiles[3])
    for ref in (gpad, hpad):
        for j in (0, 1, 6, 7):
            ref[j] = zero
    acc1[...] = jnp.zeros_like(acc1)
    acc2[...] = jnp.zeros_like(acc2)

    def brick(n, _):
        build_columns(xt, ex0, ex3, lx, ux, links_ref, n, t_buf, dx, mats)
        build_columns(yt, ey0, ey3, ly, uy, links_ref, n, t_buf, dd, mats)
        hidden = []
        grads = []
        for j in range(TILES):
            pre = jnp.dot(
                k1_ref[...], dx[n, j : j + 3].reshape(TAPS * C, LANES), preferred_element_type=F32
            )
            grad_hidden = jnp.dot(
                f2_ref[...], dd[n, j : j + 3].reshape(TAPS * C, LANES), preferred_element_type=F32
            )
            sigma = 1.0 / (1.0 + jnp.exp(-pre))
            hid = (pre * sigma).astype(BF)
            gpre = (grad_hidden * (sigma * (1.0 + pre * (1.0 - sigma)))).astype(BF)
            h_out[n, j] = hid
            g_out[n, j] = gpre
            hpad[j + 2] = hid
            gpad[j + 2] = gpre
            hidden.append(hid)
            grads.append(gpre)
        down, back = halo_pack(hidden, grads, lo)
        down_out[n] = down
        back_out[n] = back
        for acc, cols, pad, flip in ((acc1, dx, gpad, False), (acc2, dd, hpad, True)):
            total = acc[...]
            for k in (0, 2, 4):
                left = jnp.concatenate([cols[n, k], cols[n, k + 1]], axis=1)

                def right(at):
                    if flip:
                        return jnp.concatenate([pad[at + 1], pad[at], zero, pad[at + 2]], axis=0)
                    return jnp.concatenate([pad[at], pad[at + 1], pad[at + 2], zero], axis=0)

                both = jnp.concatenate([right(k), right(k + 1)], axis=1)
                total = total + lax.dot_general(
                    left, both, (((1,), (1,)), ((), ())), preferred_element_type=F32
                )
            acc[...] = total
        return 0

    lax.fori_loop(0, HOME, brick, 0)
    wide = lane_ids(9 * C) < 64
    first_a, first_b = acc1[:, 0:LANES], acc1[:, LANES : 2 * LANES]
    second_a, second_b = acc2[:, 0:LANES], acc2[:, LANES : 2 * LANES]
    parts = (
        jnp.where(wide, first_b, second_b),
        jnp.where(wide, second_a, first_a),
        jnp.where(wide, first_a, second_a),
    )
    for tap in range(2 * 16):
        if tap < TAPS:
            at = tap % 9 * C
            sums_out[tap // 16, tap % 16] = parts[tap // 9][at : at + C].astype(BF)
        else:
            sums_out[tap // 16, tap % 16] = zero


def second_kernel(
    space, x_ref, dy_ref, h_ref, g_ref, down_ref, back_ref, sums_ref, links_ref, count_ref,
    k2_ref, f1_ref, sq_ref, sr_ref, sc_ref,
    out_ref, grad_ref, arrived, total_ref,
    ht, gt, eh0, eh3, eg0, eg3, lh, lg, uh, ug, t_buf, dh, dg,
    low_in, up_in, r0, s1, r1, p2, r2, q_buf, a2, chunk,
    hs, hr, s0s, s0r, s1s, s1r, s2s, s2r, g2s, g2r, g1s, g1r, g0s, g0r, obs, obr,
):
    batch = lax.axis_index("batch")
    at = lax.axis_index("space")
    y, z_lo = batch // 2, lax.rem(batch, 2)
    x, inner = at // 8, lax.rem(at, 8)
    z_hi, core = inner // 2, lax.rem(inner, 2)
    other = 1 - core
    g = x * 4 + y
    z = z_hi * 2 + z_lo

    def plane_peer(number):
        return (lax.rem(number, 4) * 2 + z_lo, (number // 4) * 8 + inner)

    def column_peer(number):
        return (y * 2 + lax.rem(number, 2), x * 8 + (number // 2) * 2 + core)

    def ring(step):
        return (batch, lax.rem(at + space + step, space))

    partner = (batch, x * 8 + z_hi * 2 + other)
    plane = [plane_peer(lax.rem(g + d, 16)) for d in range(1, 16)]
    column = [column_peer(lax.rem(z + d, 8)) for d in range(1, 8)]
    barrier = greet([ring(1), ring(-1), ring(-1), ring(-2), ring(-3), partner] + column + plane)

    def start(src, dst, sends, recvs, number, device):
        copy = pltpu.make_async_remote_copy(
            src_ref=src, dst_ref=dst, send_sem=sends.at[number], recv_sem=recvs.at[number],
            device_id=device, device_id_type=MESH,
        )
        copy.start()
        return copy

    lo = lane_ids(C) < 64
    clear_last(ht, eh0, eh3)
    clear_last(gt, eg0, eg3)
    for n in range(HOME):
        for src, tiles_ref, e0, e3 in ((h_ref, ht, eh0, eh3), (g_ref, gt, eg0, eg3)):
            for j in range(TILES):
                tiles_ref[n, j] = src[n, j]
            e0[n] = swap_halves(src[n, 0])
            e3[n] = swap_halves(src[n, 3])
    pl.semaphore_wait(barrier, 28)
    halo = exchange(down_ref, back_ref, low_in, up_in, hs, hr, space)
    for copy in halo:
        copy.start()
    pair = start(sums_ref.at[other], r0, s0s, s0r, 0, partner)
    pair.wait_recv()
    for d in range(16):
        place = lax.rem(g + d, 16)
        s1[place] = (sums_ref[core, place].astype(F32) + r0[place].astype(F32)).astype(BF)
    scatter = [
        start(s1.at[lax.rem(g + d, 16)], r1.at[d - 1], s1s, s1r, d - 1, plane[d - 1])
        for d in range(1, 16)
    ]
    for copy in halo:
        copy.wait_recv()
    unpack_halo(low_in, up_in, (lh, lg), (uh, ug))
    mats = (sq_ref, sr_ref, sc_ref)
    count = count_ref[0, 0]

    def brick(n, _):
        build_columns(ht, eh0, eh3, lh, uh, links_ref, n, t_buf, dh, mats)
        build_columns(gt, eg0, eg3, lg, ug, links_ref, n, t_buf, dg, mats)
        mixed = []
        backs = []
        for j in range(TILES):
            mixed.append(jnp.dot(
                k2_ref[...], dh[n, j : j + 3].reshape(TAPS * C, LANES), preferred_element_type=F32
            ))
            backs.append(jnp.dot(
                f1_ref[...], dg[n, j : j + 3].reshape(TAPS * C, LANES), preferred_element_type=F32
            ))
        live = jnp.where(n < count, 1.0, 0.0).astype(F32)
        for k, (m, b) in enumerate(zip(from_tiles(mixed, lo), from_tiles(backs, lo))):
            lanes = slice(k * LANES, (k + 1) * LANES)
            out_ref[n, :, lanes] = ((x_ref[n, :, lanes].astype(F32) + m) * live).astype(BF)
            term = b.astype(BF).astype(F32)
            grad_ref[n, :, lanes] = ((dy_ref[n, :, lanes].astype(F32) + term) * live).astype(BF)
        return 0

    lax.fori_loop(WORK_CAP, HOME, brick, 0)
    acc = s1[g].astype(F32)
    for d in range(15):
        scatter[d].wait_recv()
        acc = acc + r1[d].astype(F32)
    p2[...] = acc.reshape(8, 8, LANES)
    column_scatter = [
        start(p2.at[lax.rem(z + d, 8)], r2.at[d - 1], s2s, s2r, d - 1, column[d - 1])
        for d in range(1, 8)
    ]
    bricks = [
        start(out_ref.at[WORK_CAP + k], arrived.at[k], obs, obr, k, ring(k + 1)) for k in range(3)
    ]
    lax.fori_loop(0, WORK_CAP, brick, 0)
    piece = p2[z]
    for d in range(7):
        column_scatter[d].wait_recv()
        piece = piece + r2[d]
    q_buf[...] = piece
    a2[z] = piece
    column_gather = [
        start(q_buf, a2.at[z], g2s, g2r, d - 1, column[d - 1]) for d in range(1, 8)
    ]
    for d in range(7):
        column_gather[d].wait_recv()
    whole = a2[...].reshape(C, LANES).astype(BF)
    chunk[...] = whole
    total_ref[core, g] = whole
    gather = [
        start(chunk, total_ref.at[core, g], g1s, g1r, d - 1, plane[d - 1]) for d in range(1, 16)
    ]
    forward = [start(chunk, total_ref.at[core, g], g0s, g0r, 0, partner)]
    for d in range(1, 16):
        gather[d - 1].wait_recv()
        came = lax.rem(g + 16 - d, 16)
        forward.append(
            start(total_ref.at[core, came], total_ref.at[core, came], g0s, g0r, d, partner)
        )
    for copy in (*forward, *bricks):
        copy.wait_recv()
    for copy in (
        *halo, pair, *scatter, *column_scatter, *column_gather, *gather, *forward, *bricks
    ):
        copy.wait_send()


def finish_kernel(
    scale, total_ref, ob_ref, arrived_ref, grad_ref, work_ref, grad_out, one_ref, two_ref, total
):
    grad_out[...] = grad_ref[...]
    work_ref[0] = ob_ref[0]
    extra = (
        arrived_ref[0].astype(F32) + arrived_ref[1].astype(F32) + arrived_ref[2].astype(F32)
    )
    work_ref[1] = (ob_ref[1].astype(F32) + extra).astype(BF)
    total[...] = total_ref[...].reshape(2048, LANES).astype(F32) * scale
    lo = lane_ids(C) < 64

    def block(tap):
        return total[tap * C : (tap + 1) * C, :]

    def swapped(tap):
        return 9 <= tap < 18

    def first_block(tap):
        value = block(tap)
        return swap_halves(value) if swapped(tap) else value

    def second_block(tap, low):
        value = block(TAPS - 1 - tap)
        return value if swapped(tap) == low else swap_halves(value)

    for tile in range(14):
        tap = 2 * tile
        here = first_block(tap)
        there = second_block(tap, True)
        if tap + 1 < TAPS:
            pair = jnp.concatenate([here, first_block(tap + 1)], axis=0)
            one_ref[:, tile * LANES : (tile + 1) * LANES] = pair.T[0:C, :]
            two_ref[:, tile * LANES : (tile + 1) * LANES] = jnp.where(
                lo, there, second_block(tap + 1, False)
            )
        else:
            pair = jnp.concatenate([here, here], axis=0)
            one_ref[:, tile * LANES : tile * LANES + C] = pair.T[0:C, 0:C]
            two_ref[:, tile * LANES : tile * LANES + C] = there[:, 0:C]


def vmem():
    return pl.BlockSpec(memory_space=pltpu.VMEM)


def smem():
    return pl.BlockSpec(memory_space=pltpu.SMEM)


def bf_scratch(*shape):
    return pltpu.VMEM(shape, BF)


def field_scratch():
    tiles = [bf_scratch(HOME + 1, TILES, C, LANES)] * 2
    rows = [bf_scratch(HOME + 1, C, LANES)] * 8
    columns = [bf_scratch(SPAN * C, 4 * LANES)] + [bf_scratch(HOME, SPAN, 9 * C, LANES)] * 2
    return tiles + rows + columns


def shards(space, groups, features, cotangent, brick_count, destination, neighbours, kernel_one, kernel_two):
    x = features[0]
    dy = cotangent[0]
    mats = shift_matrices()
    halo = bf_scratch(HOME, C, LANES)
    tile_shape = jax.ShapeDtypeStruct((HOME, TILES, C, LANES), BF)
    halo_shape = jax.ShapeDtypeStruct((HOME, C, LANES), BF)
    bricks_shape = jax.ShapeDtypeStruct((HOME, C, TILES * LANES), BF)
    flip_shape = jax.ShapeDtypeStruct((C, TAPS * C), BF)
    sums_shape = jax.ShapeDtypeStruct((2, 16, C, LANES), BF)
    dma = pltpu.SemaphoreType.DMA
    low, up, flip_one, flip_two = pl.pallas_call(
        functools.partial(first_halo_kernel, space),
        out_shape=[halo_shape, halo_shape, flip_shape, flip_shape],
        in_specs=[vmem()] * 4,
        out_specs=[vmem()] * 4,
        scratch_shapes=[halo, halo, dma((2,)), dma((2,))],
        compiler_params=pltpu.CompilerParams(collective_id=0, has_side_effects=True),
    )(x, dy, kernel_one, kernel_two)
    hidden, gpre, down, back, sums = pl.pallas_call(
        first_kernel,
        out_shape=[tile_shape, tile_shape, halo_shape, halo_shape, sums_shape],
        in_specs=[vmem()] * 4 + [smem()] * 2 + [vmem()] * 5,
        out_specs=[vmem()] * 5,
        scratch_shapes=field_scratch()
        + [bf_scratch(8, C, LANES)] * 2
        + [pltpu.VMEM((9 * C, 2 * LANES), F32)] * 2,
        compiler_params=pltpu.CompilerParams(vmem_limit_bytes=VMEM_BYTES),
    )(x, dy, low, up, neighbours, brick_count, kernel_one, flip_two, *mats)
    out, grad_in, arrived, total = pl.pallas_call(
        functools.partial(second_kernel, space),
        out_shape=[
            bricks_shape, bricks_shape,
            jax.ShapeDtypeStruct((3, C, TILES * LANES), BF), sums_shape,
        ],
        in_specs=[vmem()] * 7 + [smem()] * 2 + [vmem()] * 5,
        out_specs=[vmem()] * 4,
        scratch_shapes=field_scratch()
        + [
            halo, halo,
            bf_scratch(16, C, LANES),
            bf_scratch(16, C, LANES),
            bf_scratch(15, C, LANES),
            pltpu.VMEM((8, 8, LANES), F32),
            pltpu.VMEM((7, 8, LANES), F32),
            pltpu.VMEM((8, LANES), F32),
            pltpu.VMEM((8, 8, LANES), F32),
            bf_scratch(C, LANES),
        ]
        + [dma((n,)) for n in (2, 1, 15, 7, 7, 15, 16, 3) for _ in range(2)],
        compiler_params=pltpu.CompilerParams(
            collective_id=1, has_side_effects=True, vmem_limit_bytes=VMEM_BYTES
        ),
    )(x, dy, hidden, gpre, down, back, sums, neighbours, brick_count, kernel_two, flip_one, *mats)
    scale = 1.0 / math.sqrt(groups * space * HOME * TILES * LANES)
    grad_shape = jax.ShapeDtypeStruct((C, TAPS * C), F32)
    work, grad_out, grad_one, grad_two = pl.pallas_call(
        functools.partial(finish_kernel, scale),
        out_shape=[
            jax.ShapeDtypeStruct((WORK_CAP, C, TILES * LANES), BF), bricks_shape,
            grad_shape, grad_shape,
        ],
        in_specs=[vmem()] * 4,
        out_specs=[vmem()] * 4,
        scratch_shapes=[pltpu.VMEM((2048, LANES), F32)],
        compiler_params=pltpu.CompilerParams(vmem_limit_bytes=VMEM_BYTES),
    )(total, out, arrived, grad_in)
    return work[None], grad_out[None], grad_one, grad_two


def solution(mesh):
    return jax.shard_map(
        functools.partial(shards, mesh.shape["space"], mesh.shape["batch"]),
        mesh=mesh,
        in_specs=(
            P("batch", "space", None, None),
            P("batch", "space", None, None),
            P("batch", "space"),
            P("batch", "space"),
            P("batch", None, "space"),
            P(),
            P(),
        ),
        out_specs=(P("batch", "space", None, None), P("batch", "space", None, None), P(), P()),
        check_vma=False,
    )
```

```python
import functools
import math

import jax
import jax.numpy as jnp
import numpy as np
from jax import lax
from jax.experimental import pallas as pl
from jax.experimental.pallas import tpu as pltpu
from jax.sharding import PartitionSpec as P

WORK_CAP = 2
HOME = 5
TILES = 4
SPAN = 6
C = 64
LANES = 128
TAPS = 27
VMEM_BYTES = 60 * 1024 * 1024
MESH = pl.DeviceIdType.MESH
BF = jnp.bfloat16
F32 = jnp.float32


def shift_matrices():
    def column(q, r, blocks):
        m = np.zeros((len(blocks) * LANES, LANES), np.float32)
        for half in range(2):
            for b in range(8):
                for c in range(8):
                    bb, cc = b + q, c + r
                    kind = (2 if not 0 <= cc < 8 else 0) + (1 if not 0 <= bb < 8 else 0)
                    at = blocks.index(kind) * LANES + half * 64 + (bb % 8) * 8 + cc % 8
                    m[at, half * 64 + b * 8 + c] = 1.0
        return m

    s_q = np.concatenate([column(-1, 0, [1, 0]), column(1, 0, [1, 0])], axis=1)
    s_r = np.concatenate([column(0, -1, [0, 2]), column(0, 1, [0, 2])], axis=1)
    s_c = np.concatenate(
        [column(q, r, [1, 0, 2, 3]) for q, r in ((-1, -1), (-1, 1), (1, -1), (1, 1))], axis=1
    )
    return [jnp.asarray(m, BF) for m in (s_q, s_r, s_c)]


def lane_ids(rows):
    return lax.broadcasted_iota(jnp.int32, (rows, LANES), 1)


def swap_halves(v):
    return pltpu.roll(v, 64, 1)


def to_tiles(parts, lo):
    n0, n1, n2, n3 = parts
    return [
        jnp.where(lo, n0, swap_halves(n2)),
        jnp.where(lo, swap_halves(n0), n2),
        jnp.where(lo, n1, swap_halves(n3)),
        jnp.where(lo, swap_halves(n1), n3),
    ]


def from_tiles(tiles, lo):
    f0, f1, f2, f3 = tiles
    return [
        jnp.where(lo, f0, swap_halves(f1)),
        jnp.where(lo, f2, swap_halves(f3)),
        jnp.where(lo, swap_halves(f0), f1),
        jnp.where(lo, swap_halves(f2), f3),
    ]


def pieces(value):
    return [value[:, k * LANES : (k + 1) * LANES] for k in range(TILES)]


def offset_number(p, q, r):
    number = 9 * (p + 1) + 3 * (q + 1) + (r + 1)
    return number if number < 13 else number - 1


def build_columns(fields, planes, links_ref, n, t_ref, mats):
    s_q, s_r, s_c = mats
    lane = lane_ids(C)
    lo = lane < 64
    row = (lane % 64) // 8
    col = lane % 8

    def slot(p, q, r):
        if (p, q, r) == (0, 0, 0):
            return n
        found = links_ref[0, offset_number(p, q, r), n]
        return jnp.where(found < 0, HOME, found)

    slots = {
        (p, q, r): slot(p, q, r) for p in (-1, 0, 1) for q in (-1, 0, 1) for r in (-1, 0, 1)
    }
    zero = jnp.zeros((C, LANES), BF)
    where = []
    for tiles_ref, e0_ref, e3_ref, low_ref, up_ref, d_ref in fields:

        def source(k, q, r):
            if k == 0:
                return jnp.where(lo, low_ref[slots[-1, q, r]], e3_ref[slots[0, q, r]])
            if k == SPAN - 1:
                return jnp.where(lo, e0_ref[slots[0, q, r]], up_ref[slots[1, q, r]])
            return tiles_ref[slots[0, q, r], k - 1]

        for k in planes:
            t1 = source(k, 0, 0)
            t2 = jnp.where(row == 0, source(k, 1, 0), jnp.where(row == 7, source(k, -1, 0), zero))
            t3 = jnp.where(col == 7, source(k, 0, -1), jnp.where(col == 0, source(k, 0, 1), zero))
            above = jnp.where(col == 7, source(k, -1, -1), jnp.where(col == 0, source(k, -1, 1), zero))
            below = jnp.where(col == 7, source(k, 1, -1), jnp.where(col == 0, source(k, 1, 1), zero))
            t4 = jnp.where(row == 7, above, jnp.where(row == 0, below, zero))
            rows = slice(len(where) * C, (len(where) + 1) * C)
            t_ref[rows, 0:LANES] = t2
            t_ref[rows, LANES : 2 * LANES] = t1
            t_ref[rows, 2 * LANES : 3 * LANES] = t3
            t_ref[rows, 3 * LANES : 4 * LANES] = t4
            d_ref[n, k, 4 * C : 5 * C, :] = t1
            where.append((d_ref, k))
    used = slice(0, len(where) * C)

    def put(result, order):
        packed = result.astype(BF)
        for place, qr in enumerate(order):
            for i, (d_ref, k) in enumerate(where):
                d_ref[n, k, qr * C : (qr + 1) * C, :] = packed[
                    i * C : (i + 1) * C, place * LANES : (place + 1) * LANES
                ]

    put(jnp.dot(t_ref[used, 0 : 2 * LANES], s_q[...], preferred_element_type=F32), (1, 7))
    put(jnp.dot(t_ref[used, LANES : 3 * LANES], s_r[...], preferred_element_type=F32), (3, 5))
    put(jnp.dot(t_ref[used, :], s_c[...], preferred_element_type=F32), (0, 2, 6, 8))


def halo_pack(tiles_a, tiles_b, lo):
    down = jnp.where(lo, swap_halves(tiles_a[3]), tiles_b[3])
    back = jnp.where(lo, tiles_b[0], swap_halves(tiles_a[0]))
    return down, back


def neighbours_ring(space):
    me = lax.axis_index("space")
    batch = lax.axis_index("batch")
    return (batch, lax.rem(me + 1, space)), (batch, lax.rem(me + space - 1, space))


def exchange(down_ref, back_ref, low_ref, up_ref, send_sem, recv_sem, space):
    following, previous = neighbours_ring(space)
    forward = pltpu.make_async_remote_copy(
        src_ref=down_ref, dst_ref=low_ref, send_sem=send_sem.at[0], recv_sem=recv_sem.at[0],
        device_id=following, device_id_type=MESH,
    )
    backward = pltpu.make_async_remote_copy(
        src_ref=back_ref, dst_ref=up_ref, send_sem=send_sem.at[1], recv_sem=recv_sem.at[1],
        device_id=previous, device_id_type=MESH,
    )
    return forward, backward


def greet(devices):
    barrier = pltpu.get_barrier_semaphore()
    for device in devices:
        pl.semaphore_signal(barrier, inc=1, device_id=device, device_id_type=MESH)
    return barrier


def flip_kernels(k1_ref, k2_ref, f1_ref, f2_ref):
    lo = lane_ids(C) < 64

    def turned(tile):
        lanes = slice(tile * LANES, min((tile + 1) * LANES, TAPS * C))
        stacked = jnp.concatenate([k1_ref[:, lanes], k2_ref[:, lanes]], axis=0).astype(F32)
        if stacked.shape[1] < LANES:
            stacked = jnp.concatenate([stacked, stacked], axis=1)
        return stacked.T

    later = turned(13)
    for tile in range(14):
        here = later[0:C]
        if tile < 13:
            later = turned(12 - tile)
            next_one = later[C : 2 * C]
            lanes = slice(tile * LANES, (tile + 1) * LANES)
            f1_ref[:, lanes] = jnp.where(lo, here, swap_halves(next_one)).astype(BF)
            f2_ref[:, lanes] = jnp.where(lo, swap_halves(here), next_one).astype(BF)
        else:
            lanes = slice(tile * LANES, TAPS * C)
            f1_ref[:, lanes] = here[:, 0:C].astype(BF)
            f2_ref[:, lanes] = swap_halves(here)[:, 0:C].astype(BF)


def unpack_halo(low_in, up_in, lows, ups):
    for n in range(HOME):
        lows[0][n] = low_in[n]
        lows[1][n] = swap_halves(low_in[n])
        ups[0][n] = up_in[n]
        ups[1][n] = swap_halves(up_in[n])
    zero = jnp.zeros((C, LANES), BF)
    for ref in (*lows, *ups):
        ref[HOME] = zero


def clear_last(tiles_ref, e0_ref, e3_ref):
    zero = jnp.zeros((C, LANES), BF)
    for j in range(TILES):
        tiles_ref[HOME, j] = zero
    e0_ref[HOME] = zero
    e3_ref[HOME] = zero


INNER = (1, 2, 3, 4)
EDGE = (0, 5)


def hops(step, size):
    return min(step, size - step)


def block_kernel(
    space, x_ref, dy_ref, links_ref, count_ref, k1_hbm, k2_hbm, sq_hbm, sr_hbm, sc_hbm,
    out_ref, grad_ref, arrived, total_ref,
    xt, yt, ex0, ex3, ey0, ey3, lx, ly, ux, uy,
    ht, gt, eh0, eh3, eg0, eg3, lh, lg, uh, ug,
    t_buf, dx, dd, gpad, hpad, acc1, acc2,
    k1_ref, k2_ref, sq_ref, sr_ref, sc_ref, f1_ref, f2_ref,
    down1, back1, down2, back2, low1, up1, low2, up2, sums32, sums16,
    r0, s1, r1, p2, r2, q_buf, a2, chunk,
    local, h1s, h1r, h2s, h2r, s0s, s0r, s1s, s1r, s2s, s2r, g2s, g2r, g1s, g1r, g0s, g0r, obs, obr,
):
    batch = lax.axis_index("batch")
    at = lax.axis_index("space")
    y, z_lo = batch // 2, lax.rem(batch, 2)
    x, inner = at // 8, lax.rem(at, 8)
    z_hi, core = inner // 2, lax.rem(inner, 2)
    other = 1 - core
    g = x * 4 + y
    z = z_hi * 2 + z_lo

    def ring(step):
        return (batch, lax.rem(at + space + step, space))

    def plane_at(step, sign=1):
        px = lax.rem(x + 4 + sign * (step // 4), 4)
        py = lax.rem(y + 4 + sign * (step % 4), 4)
        return px, py

    def plane_place(step, sign=1):
        px, py = plane_at(step, sign)
        return px * 4 + py

    def plane_peer(step):
        px, py = plane_at(step)
        return (py * 2 + z_lo, px * 8 + inner)

    def column_place(step):
        return lax.rem(z + step, 8)

    def column_peer(step):
        pz = column_place(step)
        return (y * 2 + lax.rem(pz, 2), x * 8 + (pz // 2) * 2 + core)

    near_plane = sorted(range(1, 16), key=lambda i: (hops(i // 4, 4) + hops(i % 4, 4), i))
    near_column = sorted(range(1, 8), key=lambda i: (hops(i, 8), i))
    far_plane, far_column = near_plane[::-1], near_column[::-1]
    partner = (batch, x * 8 + z_hi * 2 + other)
    barrier = greet(
        [ring(1), ring(-1), ring(-1), ring(-2), ring(-3), partner]
        + [column_peer(i) for i in far_column]
        + [plane_peer(i) for i in far_plane]
    )
    loads = [
        pltpu.make_async_copy(src, dst, local.at[i])
        for i, (src, dst) in enumerate(
            ((k1_hbm, k1_ref), (k2_hbm, k2_ref), (sq_hbm, sq_ref), (sr_hbm, sr_ref), (sc_hbm, sc_ref))
        )
    ]
    for load in loads:
        load.start()

    def start(src, dst, sends, recvs, number, device):
        copy = pltpu.make_async_remote_copy(
            src_ref=src, dst_ref=dst, send_sem=sends.at[number], recv_sem=recvs.at[number],
            device_id=device, device_id_type=MESH,
        )
        copy.start()
        return copy

    lo = lane_ids(C) < 64
    zero = jnp.zeros((C, LANES), BF)
    mats = (sq_ref, sr_ref, sc_ref)
    count = count_ref[0, 0]
    for n in range(HOME):
        first_x, first_dy = x_ref[n, :, 0:LANES], dy_ref[n, :, 0:LANES]
        last_x, last_dy = x_ref[n, :, 3 * LANES :], dy_ref[n, :, 3 * LANES :]
        down1[n] = jnp.where(lo, swap_halves(last_x), last_dy)
        back1[n] = jnp.where(lo, first_dy, swap_halves(first_x))
    pl.semaphore_wait(barrier, 28)
    halo1 = exchange(down1, back1, low1, up1, h1s, h1r, space)
    for copy in halo1:
        copy.start()

    for tiles_ref, e0, e3 in ((xt, ex0, ex3), (yt, ey0, ey3), (ht, eh0, eh3), (gt, eg0, eg3)):
        clear_last(tiles_ref, e0, e3)
    for n in range(HOME):
        live = jnp.where(n < count, 1.0, 0.0).astype(F32)
        for src, tiles_ref, e0, e3 in ((x_ref, xt, ex0, ex3), (dy_ref, yt, ey0, ey3)):
            masked = (src[n].astype(F32) * live).astype(BF)
            tiles = to_tiles(pieces(masked), lo)
            for j in range(TILES):
                tiles_ref[n, j] = tiles[j]
            e0[n] = swap_halves(tiles[0])
            e3[n] = swap_halves(tiles[3])
    for ref in (gpad, hpad):
        for j in (0, 1, 6, 7):
            ref[j] = zero
    acc1[...] = jnp.zeros_like(acc1)
    acc2[...] = jnp.zeros_like(acc2)
    for load in loads:
        load.wait()
    field_x = (xt, ex0, ex3, lx, ux, dx)
    field_y = (yt, ey0, ey3, ly, uy, dd)
    field_h = (ht, eh0, eh3, lh, uh, dx)
    field_g = (gt, eg0, eg3, lg, ug, dd)

    def first_inner(n, _):
        build_columns((field_x, field_y), INNER, links_ref, n, t_buf, mats)
        return 0

    lax.fori_loop(0, HOME, first_inner, 0)
    flip_kernels(k1_ref, k2_ref, f1_ref, f2_ref)
    for copy in halo1:
        copy.wait_recv()
    unpack_halo(low1, up1, (lx, ly), (ux, uy))

    def first_brick(n, _):
        build_columns((field_x, field_y), EDGE, links_ref, n, t_buf, mats)
        hidden = []
        grads = []
        for j in range(TILES):
            pre = jnp.dot(
                k1_ref[...], dx[n, j : j + 3].reshape(TAPS * C, LANES), preferred_element_type=F32
            )
            grad_hidden = jnp.dot(
                f2_ref[...], dd[n, j : j + 3].reshape(TAPS * C, LANES), preferred_element_type=F32
            )
            sigma = 1.0 / (1.0 + jnp.exp(-pre))
            hid = (pre * sigma).astype(BF)
            gpre = (grad_hidden * (sigma * (1.0 + pre * (1.0 - sigma)))).astype(BF)
            ht[n, j] = hid
            gt[n, j] = gpre
            hpad[j + 2] = hid
            gpad[j + 2] = gpre
            hidden.append(hid)
            grads.append(gpre)
        for tiles, e0, e3 in ((hidden, eh0, eh3), (grads, eg0, eg3)):
            e0[n] = swap_halves(tiles[0])
            e3[n] = swap_halves(tiles[3])
        down, back = halo_pack(hidden, grads, lo)
        down2[n] = down
        back2[n] = back
        for acc, cols, pad, flip in ((acc1, dx, gpad, False), (acc2, dd, hpad, True)):
            total = acc[...]
            for k in (0, 2, 4):
                left = jnp.concatenate([cols[n, k], cols[n, k + 1]], axis=1)

                def right(at):
                    if flip:
                        return jnp.concatenate([pad[at + 1], pad[at], zero, pad[at + 2]], axis=0)
                    return jnp.concatenate([pad[at], pad[at + 1], pad[at + 2], zero], axis=0)

                both = jnp.concatenate([right(k), right(k + 1)], axis=1)
                total = total + lax.dot_general(
                    left, both, (((1,), (1,)), ((), ())), preferred_element_type=F32
                )
            acc[...] = total
        return 0

    lax.fori_loop(0, HOME, first_brick, 0)
    wide = lane_ids(9 * C) < 64
    first_a, first_b = acc1[:, 0:LANES], acc1[:, LANES : 2 * LANES]
    second_a, second_b = acc2[:, 0:LANES], acc2[:, LANES : 2 * LANES]
    parts = (
        jnp.where(wide, first_b, second_b),
        jnp.where(wide, second_a, first_a),
        jnp.where(wide, first_a, second_a),
    )
    for tap in range(2 * 16):
        if tap < TAPS:
            row = tap % 9 * C
            value = parts[tap // 9][row : row + C]
        else:
            value = jnp.zeros((C, LANES), F32)
        sums32[tap // 16, tap % 16] = value
        sums16[tap // 16, tap % 16] = value.astype(BF)
    pair = start(sums16.at[other], r0, s0s, s0r, 0, partner)
    halo2 = exchange(down2, back2, low2, up2, h2s, h2r, space)
    for copy in halo2:
        copy.start()

    def second_inner(n, _):
        build_columns((field_h, field_g), INNER, links_ref, n, t_buf, mats)
        return 0

    lax.fori_loop(0, WORK_CAP, second_inner, 0)
    pair.wait_recv()
    for d in far_plane + [0]:
        place = plane_place(d)
        s1[place] = (sums32[core, place] + r0[place].astype(F32)).astype(BF)
    scatter = {
        d: start(s1.at[plane_place(d)], r1.at[d - 1], s1s, s1r, d - 1, plane_peer(d))
        for d in far_plane
    }
    lax.fori_loop(WORK_CAP, HOME, second_inner, 0)
    for copy in halo2:
        copy.wait_recv()
    unpack_halo(low2, up2, (lh, lg), (uh, ug))

    def second_brick(n, _):
        build_columns((field_h, field_g), EDGE, links_ref, n, t_buf, mats)
        mixed = []
        backs = []
        for j in range(TILES):
            mixed.append(jnp.dot(
                k2_ref[...], dx[n, j : j + 3].reshape(TAPS * C, LANES), preferred_element_type=F32
            ))
            backs.append(jnp.dot(
                f1_ref[...], dd[n, j : j + 3].reshape(TAPS * C, LANES), preferred_element_type=F32
            ))
        live = jnp.where(n < count, 1.0, 0.0).astype(F32)
        for k, (m, b) in enumerate(zip(from_tiles(mixed, lo), from_tiles(backs, lo))):
            lanes = slice(k * LANES, (k + 1) * LANES)
            out_ref[n, :, lanes] = ((x_ref[n, :, lanes].astype(F32) + m) * live).astype(BF)
            term = b.astype(BF).astype(F32)
            grad_ref[n, :, lanes] = ((dy_ref[n, :, lanes].astype(F32) + term) * live).astype(BF)
        return 0

    lax.fori_loop(WORK_CAP, HOME, second_brick, 0)
    acc = s1[g].astype(F32)
    for d in near_plane:
        scatter[d].wait_recv()
        acc = acc + r1[d - 1].astype(F32)
    p2[...] = acc.reshape(8, 8, LANES)
    column_scatter = {
        d: start(p2.at[column_place(d)], r2.at[d - 1], s2s, s2r, d - 1, column_peer(d))
        for d in far_column
    }
    bricks = [
        start(out_ref.at[WORK_CAP + k], arrived.at[k], obs, obr, k, ring(k + 1)) for k in range(3)
    ]
    lax.fori_loop(0, WORK_CAP, second_brick, 0)
    piece = p2[z]
    for d in near_column:
        column_scatter[d].wait_recv()
        piece = piece + r2[d - 1]
    q_buf[...] = piece
    a2[z] = piece
    column_gather = {
        d: start(q_buf, a2.at[z], g2s, g2r, d - 1, column_peer(d)) for d in far_column
    }
    for d in near_column:
        column_gather[d].wait_recv()
    whole = a2[...].reshape(C, LANES).astype(BF)
    chunk[...] = whole
    total_ref[core, g] = whole
    gather = {
        d: start(chunk, total_ref.at[core, g], g1s, g1r, d - 1, plane_peer(d)) for d in far_plane
    }
    forward = [start(chunk, total_ref.at[core, g], g0s, g0r, 0, partner)]
    for d in near_plane:
        gather[d].wait_recv()
        came = plane_place(d, -1)
        forward.append(
            start(total_ref.at[core, came], total_ref.at[core, came], g0s, g0r, d, partner)
        )
    for copy in (*forward, *bricks):
        copy.wait_recv()
    for copy in (
        *halo1, *halo2, pair, *scatter.values(), *column_scatter.values(),
        *column_gather.values(), *gather.values(), *forward, *bricks,
    ):
        copy.wait_send()


def finish_kernel(
    scale, total_ref, ob_ref, arrived_ref, grad_ref, work_ref, grad_out, one_ref, two_ref, total
):
    grad_out[...] = grad_ref[...]
    work_ref[0] = ob_ref[0]
    extra = (
        arrived_ref[0].astype(F32) + arrived_ref[1].astype(F32) + arrived_ref[2].astype(F32)
    )
    work_ref[1] = (ob_ref[1].astype(F32) + extra).astype(BF)
    total[...] = total_ref[...].reshape(2048, LANES).astype(F32) * scale
    lo = lane_ids(C) < 64

    def block(tap):
        return total[tap * C : (tap + 1) * C, :]

    def swapped(tap):
        return 9 <= tap < 18

    def first_block(tap):
        value = block(tap)
        return swap_halves(value) if swapped(tap) else value

    def second_block(tap, low):
        value = block(TAPS - 1 - tap)
        return value if swapped(tap) == low else swap_halves(value)

    for tile in range(14):
        tap = 2 * tile
        here = first_block(tap)
        there = second_block(tap, True)
        if tap + 1 < TAPS:
            pair = jnp.concatenate([here, first_block(tap + 1)], axis=0)
            one_ref[:, tile * LANES : (tile + 1) * LANES] = pair.T[0:C, :]
            two_ref[:, tile * LANES : (tile + 1) * LANES] = jnp.where(
                lo, there, second_block(tap + 1, False)
            )
        else:
            pair = jnp.concatenate([here, here], axis=0)
            one_ref[:, tile * LANES : tile * LANES + C] = pair.T[0:C, 0:C]
            two_ref[:, tile * LANES : tile * LANES + C] = there[:, 0:C]


def vmem():
    return pl.BlockSpec(memory_space=pltpu.VMEM)


def smem():
    return pl.BlockSpec(memory_space=pltpu.SMEM)


def bf_scratch(*shape):
    return pltpu.VMEM(shape, BF)


def shards(space, groups, features, cotangent, brick_count, destination, neighbours, kernel_one, kernel_two):
    bricks_shape = jax.ShapeDtypeStruct((HOME, C, TILES * LANES), BF)
    sums_shape = jax.ShapeDtypeStruct((2, 16, C, LANES), BF)
    dma = pltpu.SemaphoreType.DMA
    tiles = bf_scratch(HOME + 1, TILES, C, LANES)
    rows = bf_scratch(HOME + 1, C, LANES)
    field = [tiles] * 2 + [rows] * 8
    anywhere = pl.BlockSpec(memory_space=pl.ANY)
    kernel_rows = bf_scratch(C, TAPS * C)
    out, grad_in, arrived, total = pl.pallas_call(
        functools.partial(block_kernel, space),
        out_shape=[
            bricks_shape, bricks_shape,
            jax.ShapeDtypeStruct((3, C, TILES * LANES), BF), sums_shape,
        ],
        in_specs=[vmem()] * 2 + [smem()] * 2 + [anywhere] * 5,
        out_specs=[vmem()] * 4,
        scratch_shapes=field
        + field
        + [bf_scratch(2 * TILES * C, 4 * LANES)]
        + [bf_scratch(HOME, SPAN, 9 * C, LANES)] * 2
        + [bf_scratch(8, C, LANES)] * 2
        + [pltpu.VMEM((9 * C, 2 * LANES), F32)] * 2
        + [kernel_rows] * 2
        + [bf_scratch(2 * LANES, 2 * LANES)] * 2
        + [bf_scratch(4 * LANES, 4 * LANES)]
        + [kernel_rows] * 2
        + [bf_scratch(HOME, C, LANES)] * 8
        + [pltpu.VMEM((2, 16, C, LANES), F32), bf_scratch(2, 16, C, LANES)]
        + [
            bf_scratch(16, C, LANES),
            bf_scratch(16, C, LANES),
            bf_scratch(15, C, LANES),
            pltpu.VMEM((8, 8, LANES), F32),
            pltpu.VMEM((7, 8, LANES), F32),
            pltpu.VMEM((8, LANES), F32),
            pltpu.VMEM((8, 8, LANES), F32),
            bf_scratch(C, LANES),
        ]
        + [dma((5,))]
        + [dma((n,)) for n in (2, 2, 1, 15, 7, 7, 15, 16, 3) for _ in range(2)],
        compiler_params=pltpu.CompilerParams(
            collective_id=0, has_side_effects=True, vmem_limit_bytes=VMEM_BYTES
        ),
    )(features[0], cotangent[0], neighbours, brick_count, kernel_one, kernel_two, *shift_matrices())
    scale = 1.0 / math.sqrt(groups * space * HOME * TILES * LANES)
    grad_shape = jax.ShapeDtypeStruct((C, TAPS * C), F32)
    work, grad_out, grad_one, grad_two = pl.pallas_call(
        functools.partial(finish_kernel, scale),
        out_shape=[
            jax.ShapeDtypeStruct((WORK_CAP, C, TILES * LANES), BF), bricks_shape,
            grad_shape, grad_shape,
        ],
        in_specs=[vmem()] * 4,
        out_specs=[vmem()] * 4,
        scratch_shapes=[pltpu.VMEM((2048, LANES), F32)],
        compiler_params=pltpu.CompilerParams(vmem_limit_bytes=VMEM_BYTES),
    )(total, out, arrived, grad_in)
    return work[None], grad_out[None], grad_one, grad_two


def solution(mesh):
    return jax.shard_map(
        functools.partial(shards, mesh.shape["space"], mesh.shape["batch"]),
        mesh=mesh,
        in_specs=(
            P("batch", "space", None, None),
            P("batch", "space", None, None),
            P("batch", "space"),
            P("batch", "space"),
            P("batch", None, "space"),
            P(),
            P(),
        ),
        out_specs=(P("batch", "space", None, None), P("batch", "space", None, None), P(), P()),
        check_vma=False,
    )
```

```python
import functools
import math

import jax
import jax.numpy as jnp
import numpy as np
from jax import lax
from jax.experimental import pallas as pl
from jax.experimental.pallas import tpu as pltpu
from jax.sharding import PartitionSpec as P

WORK_CAP = 2
HOME = 5
TILES = 4
SPAN = 6
C = 64
LANES = 128
TAPS = 27
VMEM_BYTES = 32 * 1024 * 1024
MESH = pl.DeviceIdType.MESH
BF = jnp.bfloat16
F32 = jnp.float32


def shift_matrices():
    def column(q, r, blocks):
        m = np.zeros((len(blocks) * LANES, LANES), np.float32)
        for half in range(2):
            for b in range(8):
                for c in range(8):
                    bb, cc = b + q, c + r
                    kind = (2 if not 0 <= cc < 8 else 0) + (1 if not 0 <= bb < 8 else 0)
                    at = blocks.index(kind) * LANES + half * 64 + (bb % 8) * 8 + cc % 8
                    m[at, half * 64 + b * 8 + c] = 1.0
        return m

    s_q = np.concatenate([column(-1, 0, [1, 0]), column(1, 0, [1, 0])], axis=1)
    s_r = np.concatenate([column(0, -1, [0, 2]), column(0, 1, [0, 2])], axis=1)
    s_c = np.concatenate(
        [column(q, r, [1, 0, 2, 3]) for q, r in ((-1, -1), (-1, 1), (1, -1), (1, 1))], axis=1
    )
    return [jnp.asarray(m, BF) for m in (s_q, s_r, s_c)]


def lane_ids(rows):
    return lax.broadcasted_iota(jnp.int32, (rows, LANES), 1)


def swap_halves(v):
    return pltpu.roll(v, 64, 1)


def to_tiles(parts, lo):
    n0, n1, n2, n3 = parts
    return [
        jnp.where(lo, n0, swap_halves(n2)),
        jnp.where(lo, swap_halves(n0), n2),
        jnp.where(lo, n1, swap_halves(n3)),
        jnp.where(lo, swap_halves(n1), n3),
    ]


def from_tiles(tiles, lo):
    f0, f1, f2, f3 = tiles
    return [
        jnp.where(lo, f0, swap_halves(f1)),
        jnp.where(lo, f2, swap_halves(f3)),
        jnp.where(lo, swap_halves(f0), f1),
        jnp.where(lo, swap_halves(f2), f3),
    ]


def pieces(value):
    return [value[:, k * LANES : (k + 1) * LANES] for k in range(TILES)]


def offset_number(p, q, r):
    number = 9 * (p + 1) + 3 * (q + 1) + (r + 1)
    return number if number < 13 else number - 1


def build_columns(fields, planes, links_ref, n, t_ref, mats):
    s_q, s_r, s_c = mats
    lane = lane_ids(C)
    lo = lane < 64
    row = (lane % 64) // 8
    col = lane % 8

    def slot(p, q, r):
        if (p, q, r) == (0, 0, 0):
            return n
        found = links_ref[n, 0, offset_number(p, q, r)]
        return jnp.where(found < 0, HOME, found)

    slots = {
        (p, q, r): slot(p, q, r) for p in (-1, 0, 1) for q in (-1, 0, 1) for r in (-1, 0, 1)
    }
    zero = jnp.zeros((C, LANES), BF)
    where = []
    for tiles_ref, e0_ref, e3_ref, low_ref, up_ref, d_ref in fields:

        def source(k, q, r):
            if k == 0:
                return jnp.where(lo, low_ref[slots[-1, q, r]], e3_ref[slots[0, q, r]])
            if k == SPAN - 1:
                return jnp.where(lo, e0_ref[slots[0, q, r]], up_ref[slots[1, q, r]])
            return tiles_ref[slots[0, q, r], k - 1]

        for k in planes:
            t1 = source(k, 0, 0)
            t2 = jnp.where(row == 0, source(k, 1, 0), jnp.where(row == 7, source(k, -1, 0), zero))
            t3 = jnp.where(col == 7, source(k, 0, -1), jnp.where(col == 0, source(k, 0, 1), zero))
            above = jnp.where(col == 7, source(k, -1, -1), jnp.where(col == 0, source(k, -1, 1), zero))
            below = jnp.where(col == 7, source(k, 1, -1), jnp.where(col == 0, source(k, 1, 1), zero))
            t4 = jnp.where(row == 7, above, jnp.where(row == 0, below, zero))
            rows = slice(len(where) * C, (len(where) + 1) * C)
            t_ref[rows, 0:LANES] = t2
            t_ref[rows, LANES : 2 * LANES] = t1
            t_ref[rows, 2 * LANES : 3 * LANES] = t3
            t_ref[rows, 3 * LANES : 4 * LANES] = t4
            d_ref[n, k, 4 * C : 5 * C, :] = t1
            where.append((d_ref, k))
    used = slice(0, len(where) * C)

    def put(result, order):
        packed = result.astype(BF)
        for place, qr in enumerate(order):
            for i, (d_ref, k) in enumerate(where):
                d_ref[n, k, qr * C : (qr + 1) * C, :] = packed[
                    i * C : (i + 1) * C, place * LANES : (place + 1) * LANES
                ]

    put(jnp.dot(t_ref[used, 0 : 2 * LANES], s_q[...], preferred_element_type=F32), (1, 7))
    put(jnp.dot(t_ref[used, LANES : 3 * LANES], s_r[...], preferred_element_type=F32), (3, 5))
    put(jnp.dot(t_ref[used, :], s_c[...], preferred_element_type=F32), (0, 2, 6, 8))


def halo_pack(tiles_a, tiles_b, lo):
    down = jnp.where(lo, swap_halves(tiles_a[3]), tiles_b[3])
    back = jnp.where(lo, tiles_b[0], swap_halves(tiles_a[0]))
    return down, back


def neighbours_ring(space):
    me = lax.axis_index("space")
    batch = lax.axis_index("batch")
    return (batch, lax.rem(me + 1, space)), (batch, lax.rem(me + space - 1, space))


def exchange(down_ref, back_ref, low_ref, up_ref, send_sem, recv_sem, space):
    following, previous = neighbours_ring(space)
    forward = pltpu.make_async_remote_copy(
        src_ref=down_ref, dst_ref=low_ref, send_sem=send_sem.at[0], recv_sem=recv_sem.at[0],
        device_id=following, device_id_type=MESH,
    )
    backward = pltpu.make_async_remote_copy(
        src_ref=back_ref, dst_ref=up_ref, send_sem=send_sem.at[1], recv_sem=recv_sem.at[1],
        device_id=previous, device_id_type=MESH,
    )
    return forward, backward


def greet(devices):
    barrier = pltpu.get_barrier_semaphore()
    for device in devices:
        pl.semaphore_signal(barrier, inc=1, device_id=device, device_id_type=MESH)
    return barrier


def flip_kernels(k1_ref, k2_ref, f1_ref, f2_ref):
    lo = lane_ids(C) < 64

    def turned(tile):
        lanes = slice(tile * LANES, min((tile + 1) * LANES, TAPS * C))
        stacked = jnp.concatenate([k1_ref[:, lanes], k2_ref[:, lanes]], axis=0).astype(F32)
        if stacked.shape[1] < LANES:
            stacked = jnp.concatenate([stacked, stacked], axis=1)
        return stacked.T

    later = turned(13)
    for tile in range(14):
        here = later[0:C]
        if tile < 13:
            later = turned(12 - tile)
            next_one = later[C : 2 * C]
            lanes = slice(tile * LANES, (tile + 1) * LANES)
            f1_ref[:, lanes] = jnp.where(lo, here, swap_halves(next_one)).astype(BF)
            f2_ref[:, lanes] = jnp.where(lo, swap_halves(here), next_one).astype(BF)
        else:
            lanes = slice(tile * LANES, TAPS * C)
            f1_ref[:, lanes] = here[:, 0:C].astype(BF)
            f2_ref[:, lanes] = swap_halves(here)[:, 0:C].astype(BF)


def unpack_halo(low_in, up_in, lows, ups):
    for n in range(HOME):
        lows[0][n] = low_in[n]
        lows[1][n] = swap_halves(low_in[n])
        ups[0][n] = up_in[n]
        ups[1][n] = swap_halves(up_in[n])
    zero = jnp.zeros((C, LANES), BF)
    for ref in (*lows, *ups):
        ref[HOME] = zero


def clear_last(tiles_ref, e0_ref, e3_ref):
    zero = jnp.zeros((C, LANES), BF)
    for j in range(TILES):
        tiles_ref[HOME, j] = zero
    e0_ref[HOME] = zero
    e3_ref[HOME] = zero


INNER = (1, 2, 3, 4)
EDGE = (0, 5)


def hops(step, size):
    return min(step, size - step)


def block_kernel(
    space, x_hbm, dy_hbm, links_hbm, count_ref, k1_hbm, k2_hbm, sq_hbm, sr_hbm, sc_hbm,
    out_ref, grad_ref, arrived, total_ref,
    xt, yt, ex0, ex3, ey0, ey3, lx, ly, ux, uy,
    ht, gt, eh0, eh3, eg0, eg3, lh, lg, uh, ug,
    t_buf, dx, dd, acc1, acc2,
    k1_ref, k2_ref, sq_ref, sr_ref, sc_ref, f1_ref, f2_ref,
    down1, back1, down2, back2, low1, up1, low2, up2, sums32, sums16,
    r0, s1, r1, p2, r2, q_buf, a2, chunk,
    x_ref, dy_ref, links_ref, local, h1s, h1r, h2s, h2r, s0s, s0r, s1s, s1r, s2s, s2r, g2s, g2r, g1s, g1r, g0s, g0r, obs, obr,
):
    batch = lax.axis_index("batch")
    at = lax.axis_index("space")
    y, z_lo = batch // 2, lax.rem(batch, 2)
    x, inner = at // 8, lax.rem(at, 8)
    z_hi, core = inner // 2, lax.rem(inner, 2)
    other = 1 - core
    g = x * 4 + y
    z = z_hi * 2 + z_lo

    def ring(step):
        return (batch, lax.rem(at + space + step, space))

    def plane_at(step, sign=1):
        px = lax.rem(x + 4 + sign * (step // 4), 4)
        py = lax.rem(y + 4 + sign * (step % 4), 4)
        return px, py

    def plane_place(step, sign=1):
        px, py = plane_at(step, sign)
        return px * 4 + py

    def plane_peer(step):
        px, py = plane_at(step)
        return (py * 2 + z_lo, px * 8 + inner)

    def column_place(step):
        return lax.rem(z + step, 8)

    def column_peer(step):
        pz = column_place(step)
        return (y * 2 + lax.rem(pz, 2), x * 8 + (pz // 2) * 2 + core)

    near_plane = sorted(range(1, 16), key=lambda i: (hops(i // 4, 4) + hops(i % 4, 4), i))
    near_column = sorted(range(1, 8), key=lambda i: (hops(i, 8), i))
    far_plane, far_column = near_plane[::-1], near_column[::-1]
    partner = (batch, x * 8 + z_hi * 2 + other)
    barrier = greet(
        [ring(1), ring(-1), ring(-1), ring(-2), ring(-3), partner]
        + [column_peer(i) for i in far_column]
        + [plane_peer(i) for i in far_plane]
    )
    loads = [
        pltpu.make_async_copy(src, dst, local.at[i])
        for i, (src, dst) in enumerate(
            ((x_hbm, x_ref), (dy_hbm, dy_ref), (links_hbm, links_ref), (k1_hbm, k1_ref), (k2_hbm, k2_ref),
             (sq_hbm, sq_ref), (sr_hbm, sr_ref), (sc_hbm, sc_ref))
        )
    ]
    for load in loads:
        load.start()

    def start(src, dst, sends, recvs, number, device):
        copy = pltpu.make_async_remote_copy(
            src_ref=src, dst_ref=dst, send_sem=sends.at[number], recv_sem=recvs.at[number],
            device_id=device, device_id_type=MESH,
        )
        copy.start()
        return copy

    lo = lane_ids(C) < 64
    zero = jnp.zeros((C, LANES), BF)
    mats = (sq_ref, sr_ref, sc_ref)
    for load in loads[:2]:
        load.wait()
    for n in range(HOME):
        first_x, first_dy = x_ref[n, :, 0:LANES], dy_ref[n, :, 0:LANES]
        last_x, last_dy = x_ref[n, :, 3 * LANES :], dy_ref[n, :, 3 * LANES :]
        down1[n] = jnp.where(lo, swap_halves(last_x), last_dy)
        back1[n] = jnp.where(lo, first_dy, swap_halves(first_x))
    for tiles_ref, e0, e3 in ((xt, ex0, ex3), (yt, ey0, ey3), (ht, eh0, eh3), (gt, eg0, eg3)):
        clear_last(tiles_ref, e0, e3)
    loads[2].wait()
    count = count_ref[0, 0]
    for n in range(HOME):
        live = jnp.where(n < count, 1.0, 0.0).astype(F32)
        for src, tiles_ref, e0, e3 in ((x_ref, xt, ex0, ex3), (dy_ref, yt, ey0, ey3)):
            masked = (src[n].astype(F32) * live).astype(BF)
            tiles = to_tiles(pieces(masked), lo)
            for j in range(TILES):
                tiles_ref[n, j] = tiles[j]
            e0[n] = swap_halves(tiles[0])
            e3[n] = swap_halves(tiles[3])
    acc1[...] = jnp.zeros_like(acc1)
    acc2[...] = jnp.zeros_like(acc2)
    field_x = (xt, ex0, ex3, lx, ux, dx)
    field_y = (yt, ey0, ey3, ly, uy, dd)
    field_h = (ht, eh0, eh3, lh, uh, dx)
    field_g = (gt, eg0, eg3, lg, ug, dd)

    def first_inner(n, _):
        build_columns((field_x, field_y), INNER, links_ref, n, t_buf, mats)
        return 0

    def first_convs(n, tiles):
        for j in tiles:
            pre = jnp.dot(
                k1_ref[...], dx[n, j : j + 3].reshape(TAPS * C, LANES), preferred_element_type=F32
            )
            grad_hidden = jnp.dot(
                f2_ref[...], dd[n, j : j + 3].reshape(TAPS * C, LANES), preferred_element_type=F32
            )
            sigma = 1.0 / (1.0 + jnp.exp(-pre))
            ht[n, j] = (pre * sigma).astype(BF)
            gt[n, j] = (grad_hidden * (sigma * (1.0 + pre * (1.0 - sigma)))).astype(BF)

    def first_middle(n, _):
        first_convs(n, (1, 2))
        return 0

    for load in loads[5:]:
        load.wait()
    lax.fori_loop(0, WORK_CAP, first_inner, 0)
    pl.semaphore_wait(barrier, 28)
    halo1 = exchange(down1, back1, low1, up1, h1s, h1r, space)
    for copy in halo1:
        copy.start()
    lax.fori_loop(WORK_CAP, HOME, first_inner, 0)
    for load in loads[3:5]:
        load.wait()
    flip_kernels(k1_ref, k2_ref, f1_ref, f2_ref)
    lax.fori_loop(0, HOME, first_middle, 0)
    for copy in halo1:
        copy.wait_recv()
    unpack_halo(low1, up1, (lx, ly), (ux, uy))

    def first_brick(n, _):
        build_columns((field_x, field_y), EDGE, links_ref, n, t_buf, mats)
        first_convs(n, (0, 3))
        hidden = [ht[n, j] for j in range(TILES)]
        grads = [gt[n, j] for j in range(TILES)]
        for tiles, e0, e3 in ((hidden, eh0, eh3), (grads, eg0, eg3)):
            e0[n] = swap_halves(tiles[0])
            e3[n] = swap_halves(tiles[3])
        down, back = halo_pack(hidden, grads, lo)
        down2[n] = down
        back2[n] = back
        edges = [zero, zero]
        hpad = edges + hidden + edges
        gpad = edges + grads + edges
        for acc, cols, pad, flip in ((acc1, dx, gpad, False), (acc2, dd, hpad, True)):
            total = acc[...]
            for k in (0, 2, 4):
                left = jnp.concatenate([cols[n, k], cols[n, k + 1]], axis=1)

                def right(at):
                    if flip:
                        return jnp.concatenate([pad[at + 1], pad[at], zero, pad[at + 2]], axis=0)
                    return jnp.concatenate([pad[at], pad[at + 1], pad[at + 2], zero], axis=0)

                both = jnp.concatenate([right(k), right(k + 1)], axis=1)
                total = total + lax.dot_general(
                    left, both, (((1,), (1,)), ((), ())), preferred_element_type=F32
                )
            acc[...] = total
        return 0

    lax.fori_loop(0, HOME, first_brick, 0)
    wide = lane_ids(9 * C) < 64
    first_a, first_b = acc1[:, 0:LANES], acc1[:, LANES : 2 * LANES]
    second_a, second_b = acc2[:, 0:LANES], acc2[:, LANES : 2 * LANES]
    parts = (
        jnp.where(wide, first_b, second_b),
        jnp.where(wide, second_a, first_a),
        jnp.where(wide, first_a, second_a),
    )
    for tap in range(2 * 16):
        if tap < TAPS:
            row = tap % 9 * C
            value = parts[tap // 9][row : row + C]
        else:
            value = jnp.zeros((C, LANES), F32)
        sums32[tap // 16, tap % 16] = value
        sums16[tap // 16, tap % 16] = value.astype(BF)
    pair = start(sums16.at[other], r0, s0s, s0r, 0, partner)
    halo2 = exchange(down2, back2, low2, up2, h2s, h2r, space)
    for copy in halo2:
        copy.start()

    def second_inner(n, _):
        build_columns((field_h, field_g), INNER, links_ref, n, t_buf, mats)
        return 0

    lax.fori_loop(0, WORK_CAP, second_inner, 0)
    pair.wait_recv()
    for d in far_plane + [0]:
        place = plane_place(d)
        s1[place] = (sums32[core, place] + r0[place].astype(F32)).astype(BF)
    scatter = {
        d: start(s1.at[plane_place(d)], r1.at[d - 1], s1s, s1r, d - 1, plane_peer(d))
        for d in far_plane
    }
    lax.fori_loop(WORK_CAP, HOME, second_inner, 0)
    for copy in halo2:
        copy.wait_recv()
    unpack_halo(low2, up2, (lh, lg), (uh, ug))

    def second_brick(n, _):
        build_columns((field_h, field_g), EDGE, links_ref, n, t_buf, mats)
        mixed = []
        backs = []
        for j in range(TILES):
            mixed.append(jnp.dot(
                k2_ref[...], dx[n, j : j + 3].reshape(TAPS * C, LANES), preferred_element_type=F32
            ))
            backs.append(jnp.dot(
                f1_ref[...], dd[n, j : j + 3].reshape(TAPS * C, LANES), preferred_element_type=F32
            ))
        live = jnp.where(n < count, 1.0, 0.0).astype(F32)
        for k, (m, b) in enumerate(zip(from_tiles(mixed, lo), from_tiles(backs, lo))):
            lanes = slice(k * LANES, (k + 1) * LANES)
            out_ref[n, :, lanes] = ((x_ref[n, :, lanes].astype(F32) + m) * live).astype(BF)
            term = b.astype(BF).astype(F32)
            grad_ref[n, :, lanes] = ((dy_ref[n, :, lanes].astype(F32) + term) * live).astype(BF)
        return 0

    lax.fori_loop(WORK_CAP, HOME, second_brick, 0)
    acc = s1[g].astype(F32)
    for d in near_plane:
        scatter[d].wait_recv()
        acc = acc + r1[d - 1].astype(F32)
    p2[...] = acc.reshape(8, 8, LANES)
    column_scatter = {
        d: start(p2.at[column_place(d)], r2.at[d - 1], s2s, s2r, d - 1, column_peer(d))
        for d in far_column
    }
    bricks = [
        start(out_ref.at[WORK_CAP + k], arrived.at[k], obs, obr, k, ring(k + 1)) for k in range(3)
    ]
    lax.fori_loop(0, WORK_CAP, second_brick, 0)
    piece = p2[z]
    for d in near_column:
        column_scatter[d].wait_recv()
        piece = piece + r2[d - 1]
    q_buf[...] = piece
    a2[z] = piece
    column_gather = {
        d: start(q_buf, a2.at[z], g2s, g2r, d - 1, column_peer(d)) for d in far_column
    }
    for d in near_column:
        column_gather[d].wait_recv()
    whole = a2[...].reshape(C, LANES).astype(BF)
    chunk[...] = whole
    total_ref[core, g] = whole
    gather = {
        d: start(chunk, total_ref.at[core, g], g1s, g1r, d - 1, plane_peer(d)) for d in far_plane
    }
    forward = [start(chunk, total_ref.at[core, g], g0s, g0r, 0, partner)]
    for d in near_plane:
        gather[d].wait_recv()
        came = plane_place(d, -1)
        forward.append(
            start(total_ref.at[core, came], total_ref.at[core, came], g0s, g0r, d, partner)
        )
    for copy in (*forward, *bricks):
        copy.wait_recv()
    for copy in (
        *halo1, *halo2, pair, *scatter.values(), *column_scatter.values(),
        *column_gather.values(), *gather.values(), *forward, *bricks,
    ):
        copy.wait_send()


def finish_kernel(
    scale, total_ref, ob_ref, arrived_ref, grad_ref, work_ref, grad_out, one_ref, two_ref, total
):
    grad_out[...] = grad_ref[...]
    work_ref[0] = ob_ref[0]
    extra = (
        arrived_ref[0].astype(F32) + arrived_ref[1].astype(F32) + arrived_ref[2].astype(F32)
    )
    work_ref[1] = (ob_ref[1].astype(F32) + extra).astype(BF)
    total[...] = total_ref[...].reshape(2048, LANES).astype(F32) * scale
    lo = lane_ids(C) < 64

    def block(tap):
        return total[tap * C : (tap + 1) * C, :]

    def swapped(tap):
        return 9 <= tap < 18

    def first_block(tap):
        value = block(tap)
        return swap_halves(value) if swapped(tap) else value

    def second_block(tap, low):
        value = block(TAPS - 1 - tap)
        return value if swapped(tap) == low else swap_halves(value)

    for tile in range(14):
        tap = 2 * tile
        here = first_block(tap)
        there = second_block(tap, True)
        if tap + 1 < TAPS:
            pair = jnp.concatenate([here, first_block(tap + 1)], axis=0)
            one_ref[:, tile * LANES : (tile + 1) * LANES] = pair.T[0:C, :]
            two_ref[:, tile * LANES : (tile + 1) * LANES] = jnp.where(
                lo, there, second_block(tap + 1, False)
            )
        else:
            pair = jnp.concatenate([here, here], axis=0)
            one_ref[:, tile * LANES : tile * LANES + C] = pair.T[0:C, 0:C]
            two_ref[:, tile * LANES : tile * LANES + C] = there[:, 0:C]


def vmem():
    return pl.BlockSpec(memory_space=pltpu.VMEM)


def smem():
    return pl.BlockSpec(memory_space=pltpu.SMEM)


def bf_scratch(*shape):
    return pltpu.VMEM(shape, BF)


def in_place(*values):
    return [pltpu.with_memory_space_constraint(v, pltpu.HBM) for v in values]


def shards(space, groups, features, cotangent, brick_count, destination, neighbours, kernel_one, kernel_two):
    bricks_shape = jax.ShapeDtypeStruct((HOME, C, TILES * LANES), BF)
    sums_shape = jax.ShapeDtypeStruct((2, 16, C, LANES), BF)
    dma = pltpu.SemaphoreType.DMA
    tiles = bf_scratch(HOME + 1, TILES, C, LANES)
    rows = bf_scratch(HOME + 1, C, LANES)
    field = [tiles] * 2 + [rows] * 8
    anywhere = pl.BlockSpec(memory_space=pltpu.HBM)
    kernel_rows = bf_scratch(C, TAPS * C)
    out, grad_in, arrived, total = pl.pallas_call(
        functools.partial(block_kernel, space),
        out_shape=[
            bricks_shape, bricks_shape,
            jax.ShapeDtypeStruct((3, C, TILES * LANES), BF), sums_shape,
        ],
        in_specs=[anywhere] * 3 + [smem()] + [anywhere] * 5,
        out_specs=[vmem()] * 4,
        scratch_shapes=field
        + field
        + [bf_scratch(2 * TILES * C, 4 * LANES)]
        + [bf_scratch(HOME, SPAN, 9 * C, LANES)] * 2
        + [pltpu.VMEM((9 * C, 2 * LANES), F32)] * 2
        + [kernel_rows] * 2
        + [bf_scratch(2 * LANES, 2 * LANES)] * 2
        + [bf_scratch(4 * LANES, 4 * LANES)]
        + [kernel_rows] * 2
        + [bf_scratch(HOME, C, LANES)] * 8
        + [pltpu.VMEM((2, 16, C, LANES), F32), bf_scratch(2, 16, C, LANES)]
        + [
            bf_scratch(16, C, LANES),
            bf_scratch(16, C, LANES),
            bf_scratch(15, C, LANES),
            pltpu.VMEM((8, 8, LANES), F32),
            pltpu.VMEM((7, 8, LANES), F32),
            pltpu.VMEM((8, LANES), F32),
            pltpu.VMEM((8, 8, LANES), F32),
            bf_scratch(C, LANES),
        ]
        + [bf_scratch(HOME, C, TILES * LANES)] * 2
        + [pltpu.SMEM((HOME, 1, 26), jnp.int32), dma((8,))]
        + [dma((n,)) for n in (2, 2, 1, 15, 7, 7, 15, 16, 3) for _ in range(2)],
        compiler_params=pltpu.CompilerParams(
            collective_id=0, has_side_effects=True, vmem_limit_bytes=VMEM_BYTES
        ),
    )(
        *in_place(features[0], cotangent[0], neighbours.transpose(2, 0, 1)), brick_count,
        *in_place(kernel_one, kernel_two, *shift_matrices()),
    )
    scale = 1.0 / math.sqrt(groups * space * HOME * TILES * LANES)
    grad_shape = jax.ShapeDtypeStruct((C, TAPS * C), F32)
    work, grad_out, grad_one, grad_two = pl.pallas_call(
        functools.partial(finish_kernel, scale),
        out_shape=[
            jax.ShapeDtypeStruct((WORK_CAP, C, TILES * LANES), BF), bricks_shape,
            grad_shape, grad_shape,
        ],
        in_specs=[vmem()] * 4,
        out_specs=[vmem()] * 4,
        scratch_shapes=[pltpu.VMEM((2048, LANES), F32)],
        compiler_params=pltpu.CompilerParams(vmem_limit_bytes=12 * 1024 * 1024),
    )(total, out, arrived, grad_in)
    return work[None], grad_out[None], grad_one, grad_two


def solution(mesh):
    return jax.shard_map(
        functools.partial(shards, mesh.shape["space"], mesh.shape["batch"]),
        mesh=mesh,
        in_specs=(
            P("batch", "space", None, None),
            P("batch", "space", None, None),
            P("batch", "space"),
            P("batch", "space"),
            P("batch", None, "space"),
            P(),
            P(),
        ),
        out_specs=(P("batch", "space", None, None), P("batch", "space", None, None), P(), P()),
        check_vma=False,
    )
```

```python
import functools
import math

import jax
import jax.numpy as jnp
import numpy as np
from jax import lax
from jax.experimental import pallas as pl
from jax.experimental.pallas import tpu as pltpu
from jax.sharding import PartitionSpec as P

WORK_CAP = 2
HOME = 5
TILES = 4
SPAN = 6
C = 64
LANES = 128
TAPS = 27
ROWS = 56
VMEM_BYTES = 32 * 1024 * 1024
MESH = pl.DeviceIdType.MESH
BF = jnp.bfloat16
F32 = jnp.float32


def shift_matrices():
    def column(q, r, blocks):
        m = np.zeros((len(blocks) * LANES, LANES), np.float32)
        for half in range(2):
            for b in range(8):
                for c in range(8):
                    bb, cc = b + q, c + r
                    kind = (2 if not 0 <= cc < 8 else 0) + (1 if not 0 <= bb < 8 else 0)
                    at = blocks.index(kind) * LANES + half * 64 + (bb % 8) * 8 + cc % 8
                    m[at, half * 64 + b * 8 + c] = 1.0
        return m

    s_q = np.concatenate([column(-1, 0, [1, 0]), column(1, 0, [1, 0])], axis=1)
    s_r = np.concatenate([column(0, -1, [0, 2]), column(0, 1, [0, 2])], axis=1)
    s_c = np.concatenate(
        [column(q, r, [1, 0, 2, 3]) for q, r in ((-1, -1), (-1, 1), (1, -1), (1, 1))], axis=1
    )
    return [jnp.asarray(m, BF) for m in (s_q, s_r, s_c)]


def lane_ids(rows):
    return lax.broadcasted_iota(jnp.int32, (rows, LANES), 1)


def swap_halves(v):
    return pltpu.roll(v, 64, 1)


def to_tiles(parts, lo):
    n0, n1, n2, n3 = parts
    return [
        jnp.where(lo, n0, swap_halves(n2)),
        jnp.where(lo, swap_halves(n0), n2),
        jnp.where(lo, n1, swap_halves(n3)),
        jnp.where(lo, swap_halves(n1), n3),
    ]


def from_tiles(tiles, lo):
    f0, f1, f2, f3 = tiles
    return [
        jnp.where(lo, f0, swap_halves(f1)),
        jnp.where(lo, f2, swap_halves(f3)),
        jnp.where(lo, swap_halves(f0), f1),
        jnp.where(lo, swap_halves(f2), f3),
    ]


def pieces(value):
    return [value[:, k * LANES : (k + 1) * LANES] for k in range(TILES)]


def offset_number(p, q, r):
    number = 9 * (p + 1) + 3 * (q + 1) + (r + 1)
    return number if number < 13 else number - 1


def build_columns(fields, planes, links_ref, n, t_ref, mats):
    s_q, s_r, s_c = mats
    lane = lane_ids(C)
    lo = lane < 64
    row = (lane % 64) // 8
    col = lane % 8

    def slot(p, q, r):
        if (p, q, r) == (0, 0, 0):
            return n
        found = links_ref[n, 0, offset_number(p, q, r)]
        return jnp.where(found < 0, HOME, found)

    slots = {
        (p, q, r): slot(p, q, r) for p in (-1, 0, 1) for q in (-1, 0, 1) for r in (-1, 0, 1)
    }
    zero = jnp.zeros((C, LANES), BF)
    where = []
    for tiles_ref, e0_ref, e3_ref, low_ref, up_ref, d_ref in fields:

        def source(k, q, r):
            if k == 0:
                return jnp.where(lo, low_ref[slots[-1, q, r]], e3_ref[slots[0, q, r]])
            if k == SPAN - 1:
                return jnp.where(lo, e0_ref[slots[0, q, r]], up_ref[slots[1, q, r]])
            return tiles_ref[slots[0, q, r], k - 1]

        for k in planes:
            t1 = source(k, 0, 0)
            t2 = jnp.where(row == 0, source(k, 1, 0), jnp.where(row == 7, source(k, -1, 0), zero))
            t3 = jnp.where(col == 7, source(k, 0, -1), jnp.where(col == 0, source(k, 0, 1), zero))
            above = jnp.where(col == 7, source(k, -1, -1), jnp.where(col == 0, source(k, -1, 1), zero))
            below = jnp.where(col == 7, source(k, 1, -1), jnp.where(col == 0, source(k, 1, 1), zero))
            t4 = jnp.where(row == 7, above, jnp.where(row == 0, below, zero))
            rows = slice(len(where) * C, (len(where) + 1) * C)
            t_ref[rows, 0:LANES] = t2
            t_ref[rows, LANES : 2 * LANES] = t1
            t_ref[rows, 2 * LANES : 3 * LANES] = t3
            t_ref[rows, 3 * LANES : 4 * LANES] = t4
            d_ref[n, k, 4 * C : 5 * C, :] = t1
            where.append((d_ref, k))
    used = slice(0, len(where) * C)

    def put(result, order):
        packed = result.astype(BF)
        for place, qr in enumerate(order):
            for i, (d_ref, k) in enumerate(where):
                d_ref[n, k, qr * C : (qr + 1) * C, :] = packed[
                    i * C : (i + 1) * C, place * LANES : (place + 1) * LANES
                ]

    put(jnp.dot(t_ref[used, 0 : 2 * LANES], s_q[...], preferred_element_type=F32), (1, 7))
    put(jnp.dot(t_ref[used, LANES : 3 * LANES], s_r[...], preferred_element_type=F32), (3, 5))
    put(jnp.dot(t_ref[used, :], s_c[...], preferred_element_type=F32), (0, 2, 6, 8))


def halo_pack(tiles_a, tiles_b, lo):
    down = jnp.where(lo, swap_halves(tiles_a[3]), tiles_b[3])
    back = jnp.where(lo, tiles_b[0], swap_halves(tiles_a[0]))
    return down, back


def neighbours_ring(space):
    me = lax.axis_index("space")
    batch = lax.axis_index("batch")
    return (batch, lax.rem(me + 1, space)), (batch, lax.rem(me + space - 1, space))


def exchange(down_ref, back_ref, low_ref, up_ref, send_sem, recv_sem, space):
    following, previous = neighbours_ring(space)
    forward = pltpu.make_async_remote_copy(
        src_ref=down_ref, dst_ref=low_ref, send_sem=send_sem.at[0], recv_sem=recv_sem.at[0],
        device_id=following, device_id_type=MESH,
    )
    backward = pltpu.make_async_remote_copy(
        src_ref=back_ref, dst_ref=up_ref, send_sem=send_sem.at[1], recv_sem=recv_sem.at[1],
        device_id=previous, device_id_type=MESH,
    )
    return forward, backward


def greet(devices):
    barrier = pltpu.get_barrier_semaphore()
    for device in devices:
        pl.semaphore_signal(barrier, inc=1, device_id=device, device_id_type=MESH)
    return barrier


def flip_kernels(k1_ref, k2_ref, f1_ref, f2_ref):
    lo = lane_ids(C) < 64

    def turned(tile):
        lanes = slice(tile * LANES, min((tile + 1) * LANES, TAPS * C))
        stacked = jnp.concatenate([k1_ref[:, lanes], k2_ref[:, lanes]], axis=0).astype(F32)
        if stacked.shape[1] < LANES:
            stacked = jnp.concatenate([stacked, stacked], axis=1)
        return stacked.T

    later = turned(13)
    for tile in range(14):
        here = later[0:C]
        if tile < 13:
            later = turned(12 - tile)
            next_one = later[C : 2 * C]
            lanes = slice(tile * LANES, (tile + 1) * LANES)
            f1_ref[:, lanes] = jnp.where(lo, here, swap_halves(next_one)).astype(BF)
            f2_ref[:, lanes] = jnp.where(lo, swap_halves(here), next_one).astype(BF)
        else:
            lanes = slice(tile * LANES, TAPS * C)
            f1_ref[:, lanes] = here[:, 0:C].astype(BF)
            f2_ref[:, lanes] = swap_halves(here)[:, 0:C].astype(BF)


def unpack_halo(low_in, up_in, lows, ups):
    for n in range(HOME):
        lows[0][n] = low_in[n]
        lows[1][n] = swap_halves(low_in[n])
        ups[0][n] = up_in[n]
        ups[1][n] = swap_halves(up_in[n])
    zero = jnp.zeros((C, LANES), BF)
    for ref in (*lows, *ups):
        ref[HOME] = zero


def clear_last(tiles_ref, e0_ref, e3_ref):
    zero = jnp.zeros((C, LANES), BF)
    for j in range(TILES):
        tiles_ref[HOME, j] = zero
    e0_ref[HOME] = zero
    e3_ref[HOME] = zero


INNER = (1, 2, 3, 4)
EDGE = (0, 5)


def hops(step, size):
    return min(step, size - step)


def block_kernel(
    space, x_hbm, dy_hbm, links_hbm, count_ref, k1_hbm, k2_hbm, sq_hbm, sr_hbm, sc_hbm,
    out_ref, grad_ref, arrived, total_ref,
    xt, yt, ex0, ex3, ey0, ey3, lx, ly, ux, uy,
    ht, gt, eh0, eh3, eg0, eg3, lh, lg, uh, ug,
    t_buf, dx, dd, acc1, acc2,
    k1_ref, k2_ref, sq_ref, sr_ref, sc_ref, f1_ref, f2_ref,
    down1, back1, down2, back2, low1, up1, low2, up2, flat, sums32,
    r0, s1, r1, zbuf, rz, chunk,
    x_ref, dy_ref, links_ref, local, h1s, h1r, h2s, h2r, s0s, s0r, s1s, s1r, g2s, g2r, g1s, g1r, g0s, g0r, obs, obr,
):
    batch = lax.axis_index("batch")
    at = lax.axis_index("space")
    y, z_lo = batch // 2, lax.rem(batch, 2)
    x, inner = at // 8, lax.rem(at, 8)
    z_hi, core = inner // 2, lax.rem(inner, 2)
    other = 1 - core
    g = x * 4 + y
    z = z_hi * 2 + z_lo

    def ring(step):
        return (batch, lax.rem(at + space + step, space))

    def plane_at(step, sign=1):
        px = lax.rem(x + 4 + sign * (step // 4), 4)
        py = lax.rem(y + 4 + sign * (step % 4), 4)
        return px, py

    def plane_place(step, sign=1):
        px, py = plane_at(step, sign)
        return px * 4 + py

    def plane_peer(step):
        px, py = plane_at(step)
        return (py * 2 + z_lo, px * 8 + inner)

    def column_place(step):
        return lax.rem(z + step, 8)

    def column_peer(step):
        pz = column_place(step)
        return (y * 2 + lax.rem(pz, 2), x * 8 + (pz // 2) * 2 + core)

    near_plane = sorted(range(1, 16), key=lambda i: (hops(i // 4, 4) + hops(i % 4, 4), i))
    near_column = sorted(range(1, 8), key=lambda i: (hops(i, 8), i))
    far_plane, far_column = near_plane[::-1], near_column[::-1]
    partner = (batch, x * 8 + z_hi * 2 + other)
    barrier = greet(
        [ring(1), ring(-1), ring(-1), ring(-2), ring(-3), partner]
        + [column_peer(i) for i in far_column]
        + [plane_peer(i) for i in far_plane]
    )
    loads = [
        pltpu.make_async_copy(src, dst, local.at[i])
        for i, (src, dst) in enumerate(
            ((x_hbm, x_ref), (dy_hbm, dy_ref), (links_hbm, links_ref), (k1_hbm, k1_ref), (k2_hbm, k2_ref),
             (sq_hbm, sq_ref), (sr_hbm, sr_ref), (sc_hbm, sc_ref))
        )
    ]
    for load in loads:
        load.start()

    def start(src, dst, sends, recvs, number, device):
        copy = pltpu.make_async_remote_copy(
            src_ref=src, dst_ref=dst, send_sem=sends.at[number], recv_sem=recvs.at[number],
            device_id=device, device_id_type=MESH,
        )
        copy.start()
        return copy

    lo = lane_ids(C) < 64
    zero = jnp.zeros((C, LANES), BF)
    mats = (sq_ref, sr_ref, sc_ref)
    for load in loads[:2]:
        load.wait()
    for n in range(HOME):
        first_x, first_dy = x_ref[n, :, 0:LANES], dy_ref[n, :, 0:LANES]
        last_x, last_dy = x_ref[n, :, 3 * LANES :], dy_ref[n, :, 3 * LANES :]
        down1[n] = jnp.where(lo, swap_halves(last_x), last_dy)
        back1[n] = jnp.where(lo, first_dy, swap_halves(first_x))
    for tiles_ref, e0, e3 in ((xt, ex0, ex3), (yt, ey0, ey3), (ht, eh0, eh3), (gt, eg0, eg3)):
        clear_last(tiles_ref, e0, e3)
    loads[2].wait()
    count = count_ref[0, 0]
    for n in range(HOME):
        live = jnp.where(n < count, 1.0, 0.0).astype(F32)
        for src, tiles_ref, e0, e3 in ((x_ref, xt, ex0, ex3), (dy_ref, yt, ey0, ey3)):
            masked = (src[n].astype(F32) * live).astype(BF)
            tiles = to_tiles(pieces(masked), lo)
            for j in range(TILES):
                tiles_ref[n, j] = tiles[j]
            e0[n] = swap_halves(tiles[0])
            e3[n] = swap_halves(tiles[3])
    acc1[...] = jnp.zeros_like(acc1)
    acc2[...] = jnp.zeros_like(acc2)
    field_x = (xt, ex0, ex3, lx, ux, dx)
    field_y = (yt, ey0, ey3, ly, uy, dd)
    field_h = (ht, eh0, eh3, lh, uh, dx)
    field_g = (gt, eg0, eg3, lg, ug, dd)

    def first_inner(n, _):
        build_columns((field_x, field_y), INNER, links_ref, n, t_buf, mats)
        return 0

    def first_convs(n, tiles):
        for j in tiles:
            pre = jnp.dot(
                k1_ref[...], dx[n, j : j + 3].reshape(TAPS * C, LANES), preferred_element_type=F32
            )
            grad_hidden = jnp.dot(
                f2_ref[...], dd[n, j : j + 3].reshape(TAPS * C, LANES), preferred_element_type=F32
            )
            sigma = 1.0 / (1.0 + jnp.exp(-pre))
            ht[n, j] = (pre * sigma).astype(BF)
            gt[n, j] = (grad_hidden * (sigma * (1.0 + pre * (1.0 - sigma)))).astype(BF)

    def first_middle(n, _):
        first_convs(n, (1, 2))
        return 0

    for load in loads[5:]:
        load.wait()
    lax.fori_loop(0, WORK_CAP, first_inner, 0)
    pl.semaphore_wait(barrier, 28)
    halo1 = exchange(down1, back1, low1, up1, h1s, h1r, space)
    for copy in halo1:
        copy.start()
    lax.fori_loop(WORK_CAP, HOME, first_inner, 0)
    for load in loads[3:5]:
        load.wait()
    flip_kernels(k1_ref, k2_ref, f1_ref, f2_ref)
    lax.fori_loop(0, HOME, first_middle, 0)
    for copy in halo1:
        copy.wait_recv()
    unpack_halo(low1, up1, (lx, ly), (ux, uy))

    def first_brick(n, _):
        build_columns((field_x, field_y), EDGE, links_ref, n, t_buf, mats)
        first_convs(n, (0, 3))
        hidden = [ht[n, j] for j in range(TILES)]
        grads = [gt[n, j] for j in range(TILES)]
        for tiles, e0, e3 in ((hidden, eh0, eh3), (grads, eg0, eg3)):
            e0[n] = swap_halves(tiles[0])
            e3[n] = swap_halves(tiles[3])
        down, back = halo_pack(hidden, grads, lo)
        down2[n] = down
        back2[n] = back
        edges = [zero, zero]
        hpad = edges + hidden + edges
        gpad = edges + grads + edges
        for acc, cols, pad, flip in ((acc1, dx, gpad, False), (acc2, dd, hpad, True)):
            total = acc[...]
            for k in (0, 2, 4):
                left = jnp.concatenate([cols[n, k], cols[n, k + 1]], axis=1)

                def right(at):
                    if flip:
                        return jnp.concatenate([pad[at + 1], pad[at], zero, pad[at + 2]], axis=0)
                    return jnp.concatenate([pad[at], pad[at + 1], pad[at + 2], zero], axis=0)

                both = jnp.concatenate([right(k), right(k + 1)], axis=1)
                total = total + lax.dot_general(
                    left, both, (((1,), (1,)), ((), ())), preferred_element_type=F32
                )
            acc[...] = total
        return 0

    lax.fori_loop(0, HOME, first_brick, 0)
    wide = lane_ids(9 * C) < 64
    first_a, first_b = acc1[:, 0:LANES], acc1[:, LANES : 2 * LANES]
    second_a, second_b = acc2[:, 0:LANES], acc2[:, LANES : 2 * LANES]
    parts = (
        jnp.where(wide, first_b, second_b),
        jnp.where(wide, second_a, first_a),
        jnp.where(wide, first_a, second_a),
    )
    for i, part in enumerate(parts):
        flat[i * 9 * C : (i + 1) * 9 * C, :] = part
    flat[TAPS * C :, :] = jnp.zeros((32 * ROWS - TAPS * C, LANES), F32)
    for i in range(32):
        value = flat[i * ROWS : (i + 1) * ROWS, :]
        sums32[i // 16, i % 16, 0:ROWS] = value
    pair = start(sums32.at[other, :, 0:ROWS], r0.at[:, 0:ROWS], s0s, s0r, 0, partner)
    halo2 = exchange(down2, back2, low2, up2, h2s, h2r, space)
    for copy in halo2:
        copy.start()

    def second_inner(n, _):
        build_columns((field_h, field_g), INNER, links_ref, n, t_buf, mats)
        return 0

    lax.fori_loop(0, WORK_CAP, second_inner, 0)
    pair.wait_recv()
    for d in far_plane + [0]:
        place = plane_place(d)
        s1[place, 0:ROWS] = (sums32[core, place, 0:ROWS] + r0[place, 0:ROWS]).astype(BF)
    scatter = {
        d: start(s1.at[plane_place(d), 0:ROWS], r1.at[d - 1, 0:ROWS], s1s, s1r, d - 1, plane_peer(d))
        for d in far_plane
    }
    lax.fori_loop(WORK_CAP, HOME, second_inner, 0)
    for copy in halo2:
        copy.wait_recv()
    unpack_halo(low2, up2, (lh, lg), (uh, ug))

    def second_brick(n, _):
        build_columns((field_h, field_g), EDGE, links_ref, n, t_buf, mats)
        mixed = []
        backs = []
        for j in range(TILES):
            mixed.append(jnp.dot(
                k2_ref[...], dx[n, j : j + 3].reshape(TAPS * C, LANES), preferred_element_type=F32
            ))
            backs.append(jnp.dot(
                f1_ref[...], dd[n, j : j + 3].reshape(TAPS * C, LANES), preferred_element_type=F32
            ))
        live = jnp.where(n < count, 1.0, 0.0).astype(F32)
        for k, (m, b) in enumerate(zip(from_tiles(mixed, lo), from_tiles(backs, lo))):
            lanes = slice(k * LANES, (k + 1) * LANES)
            out_ref[n, :, lanes] = ((x_ref[n, :, lanes].astype(F32) + m) * live).astype(BF)
            term = b.astype(BF).astype(F32)
            grad_ref[n, :, lanes] = ((dy_ref[n, :, lanes].astype(F32) + term) * live).astype(BF)
        return 0

    lax.fori_loop(WORK_CAP, HOME, second_brick, 0)
    acc = s1[g, 0:ROWS].astype(F32)
    for d in near_plane:
        scatter[d].wait_recv()
        acc = acc + r1[d - 1, 0:ROWS].astype(F32)
    zbuf[0:ROWS] = acc.astype(BF)
    rz[z, 0:ROWS] = acc.astype(BF)
    column_gather = {
        d: start(zbuf.at[0:ROWS], rz.at[z, 0:ROWS], g2s, g2r, d - 1, column_peer(d))
        for d in far_column
    }
    bricks = [
        start(out_ref.at[WORK_CAP + k], arrived.at[k], obs, obr, k, ring(k + 1)) for k in range(3)
    ]
    lax.fori_loop(0, WORK_CAP, second_brick, 0)
    for d in near_column:
        column_gather[d].wait_recv()
    whole = rz[0, 0:ROWS].astype(F32)
    for i in range(1, 8):
        whole = whole + rz[i, 0:ROWS].astype(F32)
    whole = whole.astype(BF)
    chunk[0:ROWS] = whole
    total_ref[core, g, 0:ROWS] = whole
    used = chunk.at[0:ROWS]
    gather = {
        d: start(used, total_ref.at[core, g, 0:ROWS], g1s, g1r, d - 1, plane_peer(d)) for d in far_plane
    }
    forward = [start(used, total_ref.at[core, g, 0:ROWS], g0s, g0r, 0, partner)]
    for d in near_plane:
        gather[d].wait_recv()
        came = plane_place(d, -1)
        forward.append(
            start(
                total_ref.at[core, came, 0:ROWS], total_ref.at[core, came, 0:ROWS], g0s, g0r, d, partner
            )
        )
    for copy in (*forward, *bricks):
        copy.wait_recv()
    for copy in (
        *halo1, *halo2, pair, *scatter.values(),
        *column_gather.values(), *gather.values(), *forward, *bricks,
    ):
        copy.wait_send()


def finish_kernel(
    scale, total_ref, ob_ref, arrived_ref, grad_ref, work_ref, grad_out, one_ref, two_ref, total
):
    grad_out[...] = grad_ref[...]
    work_ref[0] = ob_ref[0]
    extra = (
        arrived_ref[0].astype(F32) + arrived_ref[1].astype(F32) + arrived_ref[2].astype(F32)
    )
    work_ref[1] = (ob_ref[1].astype(F32) + extra).astype(BF)
    for i in range(32):
        total[i * ROWS : (i + 1) * ROWS, :] = total_ref[i // 16, i % 16, 0:ROWS].astype(F32) * scale
    lo = lane_ids(C) < 64

    def block(tap):
        return total[tap * C : (tap + 1) * C, :]

    def swapped(tap):
        return 9 <= tap < 18

    def first_block(tap):
        value = block(tap)
        return swap_halves(value) if swapped(tap) else value

    def second_block(tap, low):
        value = block(TAPS - 1 - tap)
        return value if swapped(tap) == low else swap_halves(value)

    for tile in range(14):
        tap = 2 * tile
        here = first_block(tap)
        there = second_block(tap, True)
        if tap + 1 < TAPS:
            pair = jnp.concatenate([here, first_block(tap + 1)], axis=0)
            one_ref[:, tile * LANES : (tile + 1) * LANES] = pair.T[0:C, :]
            two_ref[:, tile * LANES : (tile + 1) * LANES] = jnp.where(
                lo, there, second_block(tap + 1, False)
            )
        else:
            pair = jnp.concatenate([here, here], axis=0)
            one_ref[:, tile * LANES : tile * LANES + C] = pair.T[0:C, 0:C]
            two_ref[:, tile * LANES : tile * LANES + C] = there[:, 0:C]


def vmem():
    return pl.BlockSpec(memory_space=pltpu.VMEM)


def smem():
    return pl.BlockSpec(memory_space=pltpu.SMEM)


def bf_scratch(*shape):
    return pltpu.VMEM(shape, BF)


def in_place(*values):
    return [pltpu.with_memory_space_constraint(v, pltpu.HBM) for v in values]


def shards(space, groups, features, cotangent, brick_count, destination, neighbours, kernel_one, kernel_two):
    bricks_shape = jax.ShapeDtypeStruct((HOME, C, TILES * LANES), BF)
    sums_shape = jax.ShapeDtypeStruct((2, 16, C, LANES), BF)
    dma = pltpu.SemaphoreType.DMA
    tiles = bf_scratch(HOME + 1, TILES, C, LANES)
    rows = bf_scratch(HOME + 1, C, LANES)
    field = [tiles] * 2 + [rows] * 8
    anywhere = pl.BlockSpec(memory_space=pltpu.HBM)
    kernel_rows = bf_scratch(C, TAPS * C)
    out, grad_in, arrived, total = pl.pallas_call(
        functools.partial(block_kernel, space),
        out_shape=[
            bricks_shape, bricks_shape,
            jax.ShapeDtypeStruct((3, C, TILES * LANES), BF), sums_shape,
        ],
        in_specs=[anywhere] * 3 + [smem()] + [anywhere] * 5,
        out_specs=[vmem()] * 4,
        scratch_shapes=field
        + field
        + [bf_scratch(2 * TILES * C, 4 * LANES)]
        + [bf_scratch(HOME, SPAN, 9 * C, LANES)] * 2
        + [pltpu.VMEM((9 * C, 2 * LANES), F32)] * 2
        + [kernel_rows] * 2
        + [bf_scratch(2 * LANES, 2 * LANES)] * 2
        + [bf_scratch(4 * LANES, 4 * LANES)]
        + [kernel_rows] * 2
        + [bf_scratch(HOME, C, LANES)] * 8
        + [pltpu.VMEM((32 * ROWS, LANES), F32)]
        + [pltpu.VMEM((2, 16, C, LANES), F32), pltpu.VMEM((16, C, LANES), F32)]
        + [
            bf_scratch(16, C, LANES),
            bf_scratch(15, C, LANES),
            bf_scratch(C, LANES),
            bf_scratch(8, C, LANES),
            bf_scratch(C, LANES),
        ]
        + [bf_scratch(HOME, C, TILES * LANES)] * 2
        + [pltpu.SMEM((HOME, 1, 26), jnp.int32), dma((8,))]
        + [dma((n,)) for n in (2, 2, 1, 15, 7, 15, 16, 3) for _ in range(2)],
        compiler_params=pltpu.CompilerParams(
            collective_id=0, has_side_effects=True, vmem_limit_bytes=VMEM_BYTES
        ),
    )(
        *in_place(features[0], cotangent[0], neighbours.transpose(2, 0, 1)), brick_count,
        *in_place(kernel_one, kernel_two, *shift_matrices()),
    )
    scale = 1.0 / math.sqrt(groups * space * HOME * TILES * LANES)
    grad_shape = jax.ShapeDtypeStruct((C, TAPS * C), F32)
    work, grad_out, grad_one, grad_two = pl.pallas_call(
        functools.partial(finish_kernel, scale),
        out_shape=[
            jax.ShapeDtypeStruct((WORK_CAP, C, TILES * LANES), BF), bricks_shape,
            grad_shape, grad_shape,
        ],
        in_specs=[vmem()] * 4,
        out_specs=[vmem()] * 4,
        scratch_shapes=[pltpu.VMEM((32 * ROWS, LANES), F32)],
        compiler_params=pltpu.CompilerParams(vmem_limit_bytes=12 * 1024 * 1024),
    )(total, out, arrived, grad_in)
    return work[None], grad_out[None], grad_one, grad_two


def solution(mesh):
    return jax.shard_map(
        functools.partial(shards, mesh.shape["space"], mesh.shape["batch"]),
        mesh=mesh,
        in_specs=(
            P("batch", "space", None, None),
            P("batch", "space", None, None),
            P("batch", "space"),
            P("batch", "space"),
            P("batch", None, "space"),
            P(),
            P(),
        ),
        out_specs=(P("batch", "space", None, None), P("batch", "space", None, None), P(), P()),
        check_vma=False,
    )
```

```python
import functools
import math

import jax
import jax.numpy as jnp
import numpy as np
from jax import lax
from jax.experimental import pallas as pl
from jax.experimental.pallas import tpu as pltpu
from jax.sharding import PartitionSpec as P

WORK_CAP = 2
HOME = 5
TILES = 4
SPAN = 6
C = 64
LANES = 128
TAPS = 27
ROWS = 56
VMEM_BYTES = 32 * 1024 * 1024
MESH = pl.DeviceIdType.MESH
BF = jnp.bfloat16
F32 = jnp.float32


def shift_matrices():
    def column(q, r, blocks):
        m = np.zeros((len(blocks) * LANES, LANES), np.float32)
        for half in range(2):
            for b in range(8):
                for c in range(8):
                    bb, cc = b + q, c + r
                    kind = (2 if not 0 <= cc < 8 else 0) + (1 if not 0 <= bb < 8 else 0)
                    at = blocks.index(kind) * LANES + half * 64 + (bb % 8) * 8 + cc % 8
                    m[at, half * 64 + b * 8 + c] = 1.0
        return m

    s_q = np.concatenate([column(-1, 0, [1, 0]), column(1, 0, [1, 0])], axis=1)
    s_r = np.concatenate([column(0, -1, [0, 2]), column(0, 1, [0, 2])], axis=1)
    s_c = np.concatenate(
        [column(q, r, [1, 0, 2, 3]) for q, r in ((-1, -1), (-1, 1), (1, -1), (1, 1))], axis=1
    )
    return [jnp.asarray(m, BF) for m in (s_q, s_r, s_c)]


def lane_ids(rows):
    return lax.broadcasted_iota(jnp.int32, (rows, LANES), 1)


def swap_halves(v):
    return pltpu.roll(v, 64, 1)


def to_tiles(parts, lo):
    n0, n1, n2, n3 = parts
    return [
        jnp.where(lo, n0, swap_halves(n2)),
        jnp.where(lo, swap_halves(n0), n2),
        jnp.where(lo, n1, swap_halves(n3)),
        jnp.where(lo, swap_halves(n1), n3),
    ]


def from_tiles(tiles, lo):
    f0, f1, f2, f3 = tiles
    return [
        jnp.where(lo, f0, swap_halves(f1)),
        jnp.where(lo, f2, swap_halves(f3)),
        jnp.where(lo, swap_halves(f0), f1),
        jnp.where(lo, swap_halves(f2), f3),
    ]


def pieces(value):
    return [value[:, k * LANES : (k + 1) * LANES] for k in range(TILES)]


def offset_number(p, q, r):
    number = 9 * (p + 1) + 3 * (q + 1) + (r + 1)
    return number if number < 13 else number - 1


def build_columns(fields, planes, links_ref, n, t_ref, mats):
    s_q, s_r, s_c = mats
    lane = lane_ids(C)
    lo = lane < 64
    row = (lane % 64) // 8
    col = lane % 8

    def slot(p, q, r):
        if (p, q, r) == (0, 0, 0):
            return n
        found = links_ref[n, 0, offset_number(p, q, r)]
        return jnp.where(found < 0, HOME, found)

    slots = {
        (p, q, r): slot(p, q, r) for p in (-1, 0, 1) for q in (-1, 0, 1) for r in (-1, 0, 1)
    }
    zero = jnp.zeros((C, LANES), BF)
    where = []
    for tiles_ref, e0_ref, e3_ref, low_ref, up_ref, d_ref in fields:

        def source(k, q, r):
            if k == 0:
                return jnp.where(lo, low_ref[slots[-1, q, r]], e3_ref[slots[0, q, r]])
            if k == SPAN - 1:
                return jnp.where(lo, e0_ref[slots[0, q, r]], up_ref[slots[1, q, r]])
            return tiles_ref[slots[0, q, r], k - 1]

        for k in planes:
            t1 = source(k, 0, 0)
            t2 = jnp.where(row == 0, source(k, 1, 0), jnp.where(row == 7, source(k, -1, 0), zero))
            t3 = jnp.where(col == 7, source(k, 0, -1), jnp.where(col == 0, source(k, 0, 1), zero))
            above = jnp.where(col == 7, source(k, -1, -1), jnp.where(col == 0, source(k, -1, 1), zero))
            below = jnp.where(col == 7, source(k, 1, -1), jnp.where(col == 0, source(k, 1, 1), zero))
            t4 = jnp.where(row == 7, above, jnp.where(row == 0, below, zero))
            rows = slice(len(where) * C, (len(where) + 1) * C)
            t_ref[rows, 0:LANES] = t2
            t_ref[rows, LANES : 2 * LANES] = t1
            t_ref[rows, 2 * LANES : 3 * LANES] = t3
            t_ref[rows, 3 * LANES : 4 * LANES] = t4
            d_ref[n, k, 4 * C : 5 * C, :] = t1
            where.append((d_ref, k))
    used = slice(0, len(where) * C)

    def put(result, order):
        packed = result.astype(BF)
        for place, qr in enumerate(order):
            for i, (d_ref, k) in enumerate(where):
                d_ref[n, k, qr * C : (qr + 1) * C, :] = packed[
                    i * C : (i + 1) * C, place * LANES : (place + 1) * LANES
                ]

    put(jnp.dot(t_ref[used, 0 : 2 * LANES], s_q[...], preferred_element_type=F32), (1, 7))
    put(jnp.dot(t_ref[used, LANES : 3 * LANES], s_r[...], preferred_element_type=F32), (3, 5))
    put(jnp.dot(t_ref[used, :], s_c[...], preferred_element_type=F32), (0, 2, 6, 8))


def halo_pack(tiles_a, tiles_b, lo):
    down = jnp.where(lo, swap_halves(tiles_a[3]), tiles_b[3])
    back = jnp.where(lo, tiles_b[0], swap_halves(tiles_a[0]))
    return down, back


def neighbours_ring(space):
    me = lax.axis_index("space")
    batch = lax.axis_index("batch")
    return (batch, lax.rem(me + 1, space)), (batch, lax.rem(me + space - 1, space))


def exchange(down_ref, back_ref, low_ref, up_ref, send_sem, recv_sem, space):
    following, previous = neighbours_ring(space)
    forward = pltpu.make_async_remote_copy(
        src_ref=down_ref, dst_ref=low_ref, send_sem=send_sem.at[0], recv_sem=recv_sem.at[0],
        device_id=following, device_id_type=MESH,
    )
    backward = pltpu.make_async_remote_copy(
        src_ref=back_ref, dst_ref=up_ref, send_sem=send_sem.at[1], recv_sem=recv_sem.at[1],
        device_id=previous, device_id_type=MESH,
    )
    return forward, backward


def greet(devices):
    barrier = pltpu.get_barrier_semaphore()
    for device in devices:
        pl.semaphore_signal(barrier, inc=1, device_id=device, device_id_type=MESH)
    return barrier


def flip_kernels(k1_ref, k2_ref, f1_ref, f2_ref):
    lo = lane_ids(C) < 64

    def turned(tile):
        lanes = slice(tile * LANES, min((tile + 1) * LANES, TAPS * C))
        stacked = jnp.concatenate([k1_ref[:, lanes], k2_ref[:, lanes]], axis=0).astype(F32)
        if stacked.shape[1] < LANES:
            stacked = jnp.concatenate([stacked, stacked], axis=1)
        return stacked.T

    later = turned(13)
    for tile in range(14):
        here = later[0:C]
        if tile < 13:
            later = turned(12 - tile)
            next_one = later[C : 2 * C]
            lanes = slice(tile * LANES, (tile + 1) * LANES)
            f1_ref[:, lanes] = jnp.where(lo, here, swap_halves(next_one)).astype(BF)
            f2_ref[:, lanes] = jnp.where(lo, swap_halves(here), next_one).astype(BF)
        else:
            lanes = slice(tile * LANES, TAPS * C)
            f1_ref[:, lanes] = here[:, 0:C].astype(BF)
            f2_ref[:, lanes] = swap_halves(here)[:, 0:C].astype(BF)


def unpack_halo(low_in, up_in, lows, ups):
    for n in range(HOME):
        lows[0][n] = low_in[n]
        lows[1][n] = swap_halves(low_in[n])
        ups[0][n] = up_in[n]
        ups[1][n] = swap_halves(up_in[n])
    zero = jnp.zeros((C, LANES), BF)
    for ref in (*lows, *ups):
        ref[HOME] = zero


def clear_last(tiles_ref, e0_ref, e3_ref):
    zero = jnp.zeros((C, LANES), BF)
    for j in range(TILES):
        tiles_ref[HOME, j] = zero
    e0_ref[HOME] = zero
    e3_ref[HOME] = zero


INNER = (1, 2, 3, 4)
EDGE = (0, 5)


def hops(step, size):
    return min(step, size - step)


def block_kernel(
    space, x_hbm, dy_hbm, links_hbm, count_ref, k1_hbm, k2_hbm, sq_hbm, sr_hbm, sc_hbm,
    out_ref, grad_ref, arrived, total_ref,
    xt, yt, ex0, ex3, ey0, ey3, lx, ly, ux, uy,
    ht, gt, eh0, eh3, eg0, eg3, lh, lg, uh, ug,
    t_buf, dx, dd, acc1, acc2,
    k1_ref, k2_ref, sq_ref, sr_ref, sc_ref, f1_ref, f2_ref,
    down1, back1, down2, back2, low1, up1, low2, up2, flat, sums32,
    r0, s1, r1, zbuf, rz, chunk,
    x_ref, dy_ref, links_ref, local, h1s, h1r, h2s, h2r, s0s, s0r, s1s, s1r, g2s, g2r, g1s, g1r, g0s, g0r, obs, obr,
):
    batch = lax.axis_index("batch")
    at = lax.axis_index("space")
    y, z_lo = batch // 2, lax.rem(batch, 2)
    x, inner = at // 8, lax.rem(at, 8)
    z_hi, core = inner // 2, lax.rem(inner, 2)
    other = 1 - core
    g = x * 4 + y
    z = z_hi * 2 + z_lo

    def ring(step):
        return (batch, lax.rem(at + space + step, space))

    def plane_at(step, sign=1):
        px = lax.rem(x + 4 + sign * (step // 4), 4)
        py = lax.rem(y + 4 + sign * (step % 4), 4)
        return px, py

    def plane_place(step, sign=1):
        px, py = plane_at(step, sign)
        return px * 4 + py

    def plane_peer(step):
        px, py = plane_at(step)
        return (py * 2 + z_lo, px * 8 + inner)

    def column_place(step):
        return lax.rem(z + step, 8)

    def column_peer(step):
        pz = column_place(step)
        return (y * 2 + lax.rem(pz, 2), x * 8 + (pz // 2) * 2 + core)

    near_plane = sorted(range(1, 16), key=lambda i: (hops(i // 4, 4) + hops(i % 4, 4), i))
    near_column = sorted(range(1, 8), key=lambda i: (hops(i, 8), i))
    far_plane, far_column = near_plane[::-1], near_column[::-1]
    partner = (batch, x * 8 + z_hi * 2 + other)
    barrier = greet(
        [ring(1), ring(-1), ring(-1), ring(-2), ring(-3), partner]
        + [column_peer(i) for i in far_column]
        + [plane_peer(i) for i in far_plane]
    )
    loads = [
        pltpu.make_async_copy(src, dst, local.at[i])
        for i, (src, dst) in enumerate(
            ((x_hbm, x_ref), (dy_hbm, dy_ref), (links_hbm, links_ref), (k1_hbm, k1_ref), (k2_hbm, k2_ref),
             (sq_hbm, sq_ref), (sr_hbm, sr_ref), (sc_hbm, sc_ref))
        )
    ]
    for load in loads:
        load.start()

    def start(src, dst, sends, recvs, number, device):
        copy = pltpu.make_async_remote_copy(
            src_ref=src, dst_ref=dst, send_sem=sends.at[number], recv_sem=recvs.at[number],
            device_id=device, device_id_type=MESH,
        )
        copy.start()
        return copy

    lo = lane_ids(C) < 64
    zero = jnp.zeros((C, LANES), BF)
    mats = (sq_ref, sr_ref, sc_ref)
    for load in loads[:2]:
        load.wait()
    for n in range(HOME):
        first_x, first_dy = x_ref[n, :, 0:LANES], dy_ref[n, :, 0:LANES]
        last_x, last_dy = x_ref[n, :, 3 * LANES :], dy_ref[n, :, 3 * LANES :]
        down1[n] = jnp.where(lo, swap_halves(last_x), last_dy)
        back1[n] = jnp.where(lo, first_dy, swap_halves(first_x))
    for tiles_ref, e0, e3 in ((xt, ex0, ex3), (yt, ey0, ey3), (ht, eh0, eh3), (gt, eg0, eg3)):
        clear_last(tiles_ref, e0, e3)
    loads[2].wait()
    count = count_ref[0, 0]
    for n in range(HOME):
        live = jnp.where(n < count, 1.0, 0.0).astype(F32)
        for src, tiles_ref, e0, e3 in ((x_ref, xt, ex0, ex3), (dy_ref, yt, ey0, ey3)):
            masked = (src[n].astype(F32) * live).astype(BF)
            tiles = to_tiles(pieces(masked), lo)
            for j in range(TILES):
                tiles_ref[n, j] = tiles[j]
            e0[n] = swap_halves(tiles[0])
            e3[n] = swap_halves(tiles[3])
    acc1[...] = jnp.zeros_like(acc1)
    acc2[...] = jnp.zeros_like(acc2)
    field_x = (xt, ex0, ex3, lx, ux, dx)
    field_y = (yt, ey0, ey3, ly, uy, dd)
    field_h = (ht, eh0, eh3, lh, uh, dx)
    field_g = (gt, eg0, eg3, lg, ug, dd)

    def first_inner(n, _):
        build_columns((field_x, field_y), INNER, links_ref, n, t_buf, mats)
        return 0

    def first_convs(n, tiles):
        for j in tiles:
            pre = jnp.dot(
                k1_ref[...], dx[n, j : j + 3].reshape(TAPS * C, LANES), preferred_element_type=F32
            )
            grad_hidden = jnp.dot(
                f2_ref[...], dd[n, j : j + 3].reshape(TAPS * C, LANES), preferred_element_type=F32
            )
            sigma = 1.0 / (1.0 + jnp.exp(-pre))
            ht[n, j] = (pre * sigma).astype(BF)
            gt[n, j] = (grad_hidden * (sigma * (1.0 + pre * (1.0 - sigma)))).astype(BF)

    def first_middle(n, _):
        first_convs(n, (1, 2))
        return 0

    for load in loads[5:]:
        load.wait()
    lax.fori_loop(0, WORK_CAP, first_inner, 0)
    pl.semaphore_wait(barrier, 28)
    halo1 = exchange(down1, back1, low1, up1, h1s, h1r, space)
    for copy in halo1:
        copy.start()
    lax.fori_loop(WORK_CAP, HOME, first_inner, 0)
    for load in loads[3:5]:
        load.wait()
    flip_kernels(k1_ref, k2_ref, f1_ref, f2_ref)
    lax.fori_loop(0, HOME, first_middle, 0)
    for copy in halo1:
        copy.wait_recv()
    unpack_halo(low1, up1, (lx, ly), (ux, uy))

    def first_brick(n, _):
        build_columns((field_x, field_y), EDGE, links_ref, n, t_buf, mats)
        first_convs(n, (0, 3))
        hidden = [ht[n, j] for j in range(TILES)]
        grads = [gt[n, j] for j in range(TILES)]
        for tiles, e0, e3 in ((hidden, eh0, eh3), (grads, eg0, eg3)):
            e0[n] = swap_halves(tiles[0])
            e3[n] = swap_halves(tiles[3])
        down, back = halo_pack(hidden, grads, lo)
        down2[n] = down
        back2[n] = back
        edges = [zero, zero]
        hpad = edges + hidden + edges
        gpad = edges + grads + edges
        for acc, cols, pad, flip in ((acc1, dx, gpad, False), (acc2, dd, hpad, True)):
            total = acc[...]
            for k in (0, 2, 4):
                left = jnp.concatenate([cols[n, k], cols[n, k + 1]], axis=1)

                def right(at):
                    if flip:
                        return jnp.concatenate([pad[at + 1], pad[at], zero, pad[at + 2]], axis=0)
                    return jnp.concatenate([pad[at], pad[at + 1], pad[at + 2], zero], axis=0)

                both = jnp.concatenate([right(k), right(k + 1)], axis=1)
                total = total + lax.dot_general(
                    left, both, (((1,), (1,)), ((), ())), preferred_element_type=F32
                )
            acc[...] = total
        return 0

    lax.fori_loop(0, HOME, first_brick, 0)
    wide = lane_ids(9 * C) < 64
    first_a, first_b = acc1[:, 0:LANES], acc1[:, LANES : 2 * LANES]
    second_a, second_b = acc2[:, 0:LANES], acc2[:, LANES : 2 * LANES]
    parts = (
        jnp.where(wide, first_b, second_b),
        jnp.where(wide, second_a, first_a),
        jnp.where(wide, first_a, second_a),
    )
    for i, part in enumerate(parts):
        flat[i * 9 * C : (i + 1) * 9 * C, :] = part
    flat[TAPS * C :, :] = jnp.zeros((32 * ROWS - TAPS * C, LANES), F32)
    for i in range(32):
        value = flat[i * ROWS : (i + 1) * ROWS, :]
        sums32[i // 16, i % 16, 0:ROWS] = value
    pair = start(sums32.at[other, :, 0:ROWS], r0.at[:, 0:ROWS], s0s, s0r, 0, partner)
    halo2 = exchange(down2, back2, low2, up2, h2s, h2r, space)
    for copy in halo2:
        copy.start()

    def second_inner(n, _):
        build_columns((field_h, field_g), INNER, links_ref, n, t_buf, mats)
        return 0

    lax.fori_loop(0, WORK_CAP, second_inner, 0)
    pair.wait_recv()
    for d in far_plane + [0]:
        place = plane_place(d)
        s1[place, 0:ROWS] = (sums32[core, place, 0:ROWS] + r0[place, 0:ROWS]).astype(BF)
    scatter = {
        d: start(s1.at[plane_place(d), 0:ROWS], r1.at[d - 1, 0:ROWS], s1s, s1r, d - 1, plane_peer(d))
        for d in far_plane
    }
    lax.fori_loop(WORK_CAP, HOME, second_inner, 0)
    for copy in halo2:
        copy.wait_recv()
    unpack_halo(low2, up2, (lh, lg), (uh, ug))

    def second_brick(n, _):
        build_columns((field_h, field_g), EDGE, links_ref, n, t_buf, mats)
        mixed = []
        backs = []
        for j in range(TILES):
            mixed.append(jnp.dot(
                k2_ref[...], dx[n, j : j + 3].reshape(TAPS * C, LANES), preferred_element_type=F32
            ))
            backs.append(jnp.dot(
                f1_ref[...], dd[n, j : j + 3].reshape(TAPS * C, LANES), preferred_element_type=F32
            ))
        live = jnp.where(n < count, 1.0, 0.0).astype(F32)
        for k, (m, b) in enumerate(zip(from_tiles(mixed, lo), from_tiles(backs, lo))):
            lanes = slice(k * LANES, (k + 1) * LANES)
            out_ref[n, :, lanes] = ((x_ref[n, :, lanes].astype(F32) + m) * live).astype(BF)
            term = b.astype(BF).astype(F32)
            grad_ref[n, :, lanes] = ((dy_ref[n, :, lanes].astype(F32) + term) * live).astype(BF)
        return 0

    lax.fori_loop(WORK_CAP, HOME, second_brick, 0)
    acc = s1[g, 0:ROWS].astype(F32)
    for d in near_plane:
        scatter[d].wait_recv()
        acc = acc + r1[d - 1, 0:ROWS].astype(F32)
    zbuf[0:ROWS] = acc.astype(BF)
    rz[z, 0:ROWS] = acc.astype(BF)
    column_gather = {
        d: start(zbuf.at[0:ROWS], rz.at[z, 0:ROWS], g2s, g2r, d - 1, column_peer(d))
        for d in far_column
    }
    lax.fori_loop(0, WORK_CAP, second_brick, 0)
    bricks = [
        start(out_ref.at[WORK_CAP + k], arrived.at[k], obs, obr, k, ring(k + 1)) for k in range(3)
    ]
    for d in near_column:
        column_gather[d].wait_recv()
    whole = rz[0, 0:ROWS].astype(F32)
    for i in range(1, 8):
        whole = whole + rz[i, 0:ROWS].astype(F32)
    whole = whole.astype(BF)
    chunk[0:ROWS] = whole
    total_ref[core, g, 0:ROWS] = whole
    used = chunk.at[0:ROWS]
    gather = {
        d: start(used, total_ref.at[core, g, 0:ROWS], g1s, g1r, d - 1, plane_peer(d)) for d in far_plane
    }
    forward = [start(used, total_ref.at[core, g, 0:ROWS], g0s, g0r, 0, partner)]
    for d in near_plane:
        gather[d].wait_recv()
        came = plane_place(d, -1)
        forward.append(
            start(
                total_ref.at[core, came, 0:ROWS], total_ref.at[core, came, 0:ROWS], g0s, g0r, d, partner
            )
        )
    for copy in (*forward, *bricks):
        copy.wait_recv()
    for copy in (
        *halo1, *halo2, pair, *scatter.values(),
        *column_gather.values(), *gather.values(), *forward, *bricks,
    ):
        copy.wait_send()


def finish_kernel(
    scale, total_ref, ob_ref, arrived_ref, grad_ref, work_ref, grad_out, one_ref, two_ref, total
):
    grad_out[...] = grad_ref[...]
    work_ref[0] = ob_ref[0]
    extra = (
        arrived_ref[0].astype(F32) + arrived_ref[1].astype(F32) + arrived_ref[2].astype(F32)
    )
    work_ref[1] = (ob_ref[1].astype(F32) + extra).astype(BF)
    for i in range(32):
        total[i * ROWS : (i + 1) * ROWS, :] = total_ref[i // 16, i % 16, 0:ROWS].astype(F32) * scale
    lo = lane_ids(C) < 64

    def block(tap):
        return total[tap * C : (tap + 1) * C, :]

    def swapped(tap):
        return 9 <= tap < 18

    def first_block(tap):
        value = block(tap)
        return swap_halves(value) if swapped(tap) else value

    def second_block(tap, low):
        value = block(TAPS - 1 - tap)
        return value if swapped(tap) == low else swap_halves(value)

    for tile in range(14):
        tap = 2 * tile
        here = first_block(tap)
        there = second_block(tap, True)
        if tap + 1 < TAPS:
            pair = jnp.concatenate([here, first_block(tap + 1)], axis=0)
            one_ref[:, tile * LANES : (tile + 1) * LANES] = pair.T[0:C, :]
            two_ref[:, tile * LANES : (tile + 1) * LANES] = jnp.where(
                lo, there, second_block(tap + 1, False)
            )
        else:
            pair = jnp.concatenate([here, here], axis=0)
            one_ref[:, tile * LANES : tile * LANES + C] = pair.T[0:C, 0:C]
            two_ref[:, tile * LANES : tile * LANES + C] = there[:, 0:C]


def vmem():
    return pl.BlockSpec(memory_space=pltpu.VMEM)


def smem():
    return pl.BlockSpec(memory_space=pltpu.SMEM)


def bf_scratch(*shape):
    return pltpu.VMEM(shape, BF)


def in_place(*values):
    return [pltpu.with_memory_space_constraint(v, pltpu.HBM) for v in values]


def shards(space, groups, features, cotangent, brick_count, destination, neighbours, kernel_one, kernel_two):
    bricks_shape = jax.ShapeDtypeStruct((HOME, C, TILES * LANES), BF)
    sums_shape = jax.ShapeDtypeStruct((2, 16, C, LANES), BF)
    dma = pltpu.SemaphoreType.DMA
    tiles = bf_scratch(HOME + 1, TILES, C, LANES)
    rows = bf_scratch(HOME + 1, C, LANES)
    field = [tiles] * 2 + [rows] * 8
    anywhere = pl.BlockSpec(memory_space=pltpu.HBM)
    kernel_rows = bf_scratch(C, TAPS * C)
    out, grad_in, arrived, total = pl.pallas_call(
        functools.partial(block_kernel, space),
        out_shape=[
            bricks_shape, bricks_shape,
            jax.ShapeDtypeStruct((3, C, TILES * LANES), BF), sums_shape,
        ],
        in_specs=[anywhere] * 3 + [smem()] + [anywhere] * 5,
        out_specs=[vmem()] * 4,
        scratch_shapes=field
        + field
        + [bf_scratch(2 * TILES * C, 4 * LANES)]
        + [bf_scratch(HOME, SPAN, 9 * C, LANES)] * 2
        + [pltpu.VMEM((9 * C, 2 * LANES), F32)] * 2
        + [kernel_rows] * 2
        + [bf_scratch(2 * LANES, 2 * LANES)] * 2
        + [bf_scratch(4 * LANES, 4 * LANES)]
        + [kernel_rows] * 2
        + [bf_scratch(HOME, C, LANES)] * 8
        + [pltpu.VMEM((32 * ROWS, LANES), F32)]
        + [pltpu.VMEM((2, 16, C, LANES), F32), pltpu.VMEM((16, C, LANES), F32)]
        + [
            bf_scratch(16, C, LANES),
            bf_scratch(15, C, LANES),
            bf_scratch(C, LANES),
            bf_scratch(8, C, LANES),
            bf_scratch(C, LANES),
        ]
        + [bf_scratch(HOME, C, TILES * LANES)] * 2
        + [pltpu.SMEM((HOME, 1, 26), jnp.int32), dma((8,))]
        + [dma((n,)) for n in (2, 2, 1, 15, 7, 15, 16, 3) for _ in range(2)],
        compiler_params=pltpu.CompilerParams(
            collective_id=0, has_side_effects=True, vmem_limit_bytes=VMEM_BYTES
        ),
    )(
        *in_place(features[0], cotangent[0], neighbours.transpose(2, 0, 1)), brick_count,
        *in_place(kernel_one, kernel_two, *shift_matrices()),
    )
    scale = 1.0 / math.sqrt(groups * space * HOME * TILES * LANES)
    grad_shape = jax.ShapeDtypeStruct((C, TAPS * C), F32)
    work, grad_out, grad_one, grad_two = pl.pallas_call(
        functools.partial(finish_kernel, scale),
        out_shape=[
            jax.ShapeDtypeStruct((WORK_CAP, C, TILES * LANES), BF), bricks_shape,
            grad_shape, grad_shape,
        ],
        in_specs=[vmem()] * 4,
        out_specs=[vmem()] * 4,
        scratch_shapes=[pltpu.VMEM((32 * ROWS, LANES), F32)],
        compiler_params=pltpu.CompilerParams(vmem_limit_bytes=12 * 1024 * 1024),
    )(total, out, arrived, grad_in)
    return work[None], grad_out[None], grad_one, grad_two


def solution(mesh):
    return jax.shard_map(
        functools.partial(shards, mesh.shape["space"], mesh.shape["batch"]),
        mesh=mesh,
        in_specs=(
            P("batch", "space", None, None),
            P("batch", "space", None, None),
            P("batch", "space"),
            P("batch", "space"),
            P("batch", None, "space"),
            P(),
            P(),
        ),
        out_specs=(P("batch", "space", None, None), P("batch", "space", None, None), P(), P()),
        check_vma=False,
    )
```
